32 devices in a mesh: lat: 4 (over z), lon: 2 (over y), hid: 4 (over x, core).
Axes of the slice: x: 2, y: 2, z: 4, core: 2. Of those that a mesh axis runs over, the one named last changes fastest.
Arguments:
- grid_latent: float32 [32, 256, 512], P('lat', 'lon'), may hold values from -6 to 6
- mesh_latent: float32 [4, 2, 512, 512], P('lat', 'lon'), may hold values from -6 to 6
- grid_edge_feats: float32 [4, 2, 4, 1024], P('lat', 'lon'), may hold values from -6 to 6
- grid_senders: int32 [4, 2, 1024], P('lat', 'lon'), may hold values from 0 to 8191, as said below
- grid_receivers: int32 [4, 2, 1024], P('lat', 'lon'), may hold values from -1 to 4095, as said below
- mesh_edge_feats: float32 [4, 2, 4, 512], P('lat', 'lon'), may hold values from -6 to 6
- mesh_senders: int32 [4, 2, 512], P('lat', 'lon'), may hold values from 0 to 4095, as said below
- mesh_receivers: int32 [4, 2, 512], P('lat', 'lon'), may hold values from -1 to 4095, as said below
- edge_weight: float32 [2, 4, 512], P(None, None, 'hid'), may hold values from -1.75 to 1.75
- sender_weight: float32 [2, 512, 512], P(None, None, 'hid'), may hold values from -0.15625 to 0.15625
- receiver_weight: float32 [2, 512, 512], P(None, None, 'hid'), may hold values from -0.15625 to 0.15625
- first_bias: float32 [2, 512], P(None, 'hid'), may hold values from -1 to 1
- out_weight: float32 [2, 512, 512], P(None, 'hid'), may hold values from -4 to 4
- out_bias: float32 [2, 512], replicated, may hold values from -3 to 3
- norm_gain: float32 [2, 512], replicated, may hold values from 0.5 to 1.5
- norm_shift: float32 [2, 512], replicated, may hold values from -3 to 3
Outputs:
- mesh_out: float32 [4, 2, 512, 512], P('lat', 'lon', None, 'hid')
The draws below stay inside these ranges and needn't reach their ends.
Inputs may be any that keep to these rules, and one draw needn't show every extreme that they name: `grid_senders`: A live slot of patch (a, b) sends from a grid cell of block (a, b) or within 2 cells outside it in latitude (never past the first or last row) and in longitude (wrapping round); a padding slot names the first cell of its own block. `grid_receivers`: in each patch's block of 1024 slots the live slots come first and their receivers are nodes of that patch in non-decreasing order; -1 marks padding; in every draw some patch has all 1024 slots live. `mesh_senders`: A live slot of patch (a, b) sends from a node of patch (a + p, b + q), p and q in -1, 0, 1, with latitude never leaving the range and longitude wrapping round; a padding slot names a node of its own patch. `mesh_receivers`: in each patch's block of 512 slots the live slots come first and their receivers are nodes of that patch in non-decreasing order; -1 marks padding; in every draw some patch has all 512 slots live.
All inputs are finite; a program needn't handle non-finite values.
Results may differ from the reference program's by a relative error of at most 0.0003.
Values sent between devices are 32-bit elements; how exact they have to be, the bound alone decides.
No kernel may reach another device: no remote copies, remote signals or barrier semaphores. Data moves between devices by JAX's collectives and lax.ppermute only.
A program may use at most 64 MiB of HBM per device.

```python
import math
import jax
import jax.numpy as jnp
from jax import lax

C = 512
H = 512
EF = 4
RIM = 2
GLAT = 8
GLON = 128
M_DEV = 512
E2_DEV = 512
E1_DEV = 1024
PLAT = 4
PLON = 2
NLAT = 32
NLON = 256


def patch_frame(slot_total):
    patch_row = jnp.arange(PLAT, dtype=jnp.int32)[:, None, None]
    patch_col = jnp.arange(PLON, dtype=jnp.int32)[None, :, None]
    slot_index = jnp.arange(slot_total, dtype=jnp.int32)[None, None, :]
    return (patch_row, patch_col, slot_index)


def live_slots(key_one, patch_row, slot_index, slot_total):
    polar_row = (patch_row == 0) | (patch_row == PLAT - 1)
    drawn_live = jax.random.randint(key_one, (PLAT, PLON, 1), slot_total // 2, slot_total + 1)
    live_count = jnp.where(polar_row, slot_total, drawn_live)
    return slot_index < live_count


def step_offsets(key_one, slot_shape):
    picked = jax.random.randint(key_one, slot_shape, 0, 6)
    return (picked == 5).astype(jnp.int32) - (picked == 0).astype(jnp.int32)


def receiver_ids(key_one, active, patch_row, patch_col, slot_shape):
    local_node = jax.random.randint(key_one, slot_shape, 0, M_DEV)
    local_node = jnp.sort(jnp.where(active, local_node, M_DEV), axis=-1)
    patch_number = patch_row * PLON + patch_col
    return jnp.where(active, patch_number * M_DEV + local_node, -1).astype(jnp.int32)


def grid_links(key):
    key_list = jax.random.split(jax.random.fold_in(key, 101), 8)
    slot_shape = (PLAT, PLON, E1_DEV)
    patch_row, patch_col, slot_index = patch_frame(E1_DEV)
    active = live_slots(key_list[0], patch_row, slot_index, E1_DEV)
    lat_step = step_offsets(key_list[1], slot_shape)
    lat_step = jnp.where((patch_row + lat_step < 0) | (patch_row + lat_step >= PLAT), 0, lat_step)
    lon_step = step_offsets(key_list[2], slot_shape)
    inner_row = jax.random.randint(key_list[3], slot_shape, 0, GLAT)
    inner_col = jax.random.randint(key_list[4], slot_shape, 0, GLON)
    rim_row = jax.random.randint(key_list[5], slot_shape, 0, RIM)
    rim_col = jax.random.randint(key_list[6], slot_shape, 0, RIM)
    cell_row = jnp.where(lat_step == 0, patch_row * GLAT + inner_row, jnp.where(lat_step < 0, patch_row * GLAT - 1 - rim_row, (patch_row + 1) * GLAT + rim_row))
    cell_col = jnp.where(lon_step == 0, patch_col * GLON + inner_col, jnp.where(lon_step < 0, patch_col * GLON - 1 - rim_col, (patch_col + 1) * GLON + rim_col)) % NLON
    senders = jnp.where(active, cell_row * NLON + cell_col, patch_row * GLAT * NLON + patch_col * GLON).astype(jnp.int32)
    receivers = receiver_ids(key_list[7], active, patch_row, patch_col, slot_shape)
    return (senders, receivers)


def mesh_links(key):
    key_list = jax.random.split(jax.random.fold_in(key, 202), 5)
    slot_shape = (PLAT, PLON, E2_DEV)
    patch_row, patch_col, slot_index = patch_frame(E2_DEV)
    active = live_slots(key_list[0], patch_row, slot_index, E2_DEV)
    lat_step = step_offsets(key_list[1], slot_shape)
    lat_step = jnp.where((patch_row + lat_step < 0) | (patch_row + lat_step >= PLAT), 0, lat_step)
    lon_step = step_offsets(key_list[2], slot_shape)
    source_row = patch_row + jnp.where(active, lat_step, 0)
    source_col = (patch_col + jnp.where(active, lon_step, 0)) % PLON
    source_node = jax.random.randint(key_list[3], slot_shape, 0, M_DEV)
    senders = ((source_row * PLON + source_col) * M_DEV + source_node).astype(jnp.int32)
    receivers = receiver_ids(key_list[4], active, patch_row, patch_col, slot_shape)
    return (senders, receivers)


def draw_grid_senders(key, part):
    return grid_links(key)[0]


def draw_grid_receivers(key, part):
    return grid_links(key)[1]


def draw_mesh_senders(key, part):
    return mesh_links(key)[0]


def draw_mesh_receivers(key, part):
    return mesh_links(key)[1]


def draw_out_weight(key, part):
    key_list = jax.random.split(jax.random.fold_in(key, 303), 3)
    spread = math.log(10.0) / 2.0
    row_scale = jnp.exp(jax.random.uniform(key_list[0], (2, H, 1), minval=-spread, maxval=spread))
    col_scale = jnp.exp(jax.random.uniform(key_list[1], (2, 1, C), minval=-spread, maxval=spread))
    values = jnp.clip(jax.random.normal(key_list[2], (2, H, C)), -2.5, 2.5) * row_scale * col_scale
    return (values / math.sqrt(H)).astype(jnp.float32)


def shard_levels(rng, dims, cuts, low, high):
    factor_of = 1.0
    for axis_at, blocks in cuts:
        heights = jax.random.uniform(jax.random.fold_in(jax.random.fold_in(rng, 6), axis_at), (blocks,), jnp.float32, low / len(cuts), high / len(cuts))
        factor_of = factor_of * jnp.repeat(jnp.exp(heights), dims[axis_at] // blocks).reshape((-1,) + (1,) * (len(dims) - 1 - axis_at))
    return factor_of


def noise(rng, dims, deviation, limit, cuts=(), held_as=jnp.bfloat16):
    values = jax.random.normal(rng, dims, jnp.float32) * deviation
    if len(cuts) > 0:
        values = shard_levels(rng, dims, cuts, -0.22, 0.18) * values
    return jnp.clip(values, min=-limit, max=limit).astype(held_as)


def setup_inputs(seed: int = 0) -> dict:
    seeds = jax.random.split(jax.random.key(seed), 17)
    return {
        "grid_latent": noise(seeds[0], (NLAT, NLON, C), 1.0, 6.0, ((0, 4), (1, 2)), jnp.float32),
        "mesh_latent": noise(seeds[1], (PLAT, PLON, M_DEV, C), 1.0, 6.0, ((0, 4), (1, 2)), jnp.float32),
        "grid_edge_feats": noise(seeds[2], (PLAT, PLON, EF, E1_DEV), 1.0, 6.0, ((0, 4), (1, 2)), jnp.float32),
        "grid_senders": draw_grid_senders(jax.random.fold_in(seeds[16], 71), 0),
        "grid_receivers": draw_grid_receivers(jax.random.fold_in(seeds[16], 71), 0),
        "mesh_edge_feats": noise(seeds[5], (PLAT, PLON, EF, E2_DEV), 1.0, 6.0, ((0, 4), (1, 2)), jnp.float32),
        "mesh_senders": draw_mesh_senders(jax.random.fold_in(seeds[16], 71), 0),
        "mesh_receivers": draw_mesh_receivers(jax.random.fold_in(seeds[16], 71), 0),
        "edge_weight": noise(seeds[8], (2, EF, H), (3 * EF) ** -0.5, 1.75, ((2, 4),), jnp.float32),
        "sender_weight": noise(seeds[9], (2, C, H), (3 * C) ** -0.5, 0.15625, ((2, 4),), jnp.float32),
        "receiver_weight": noise(seeds[10], (2, C, H), (3 * C) ** -0.5, 0.15625, ((2, 4),), jnp.float32),
        "first_bias": jnp.clip(jax.random.uniform(seeds[11], (2, H), jnp.float32, -1.0, 1.0) * shard_levels(seeds[11], (2, H), ((1, 4),), -0.4, 0.0), -1.0, 1.0),
        "out_weight": draw_out_weight(jax.random.fold_in(seeds[16], 71), 0),
        "out_bias": noise(seeds[13], (2, C), 0.5, 3.0, (), jnp.float32),
        "norm_gain": jnp.clip(jax.random.uniform(seeds[14], (2, C), jnp.float32, 0.5, 1.5), 0.5, 1.5),
        "norm_shift": noise(seeds[15], (2, C), 0.5, 3.0, (), jnp.float32),
    }


HIGHEST = lax.Precision.HIGHEST
epsilon = 1e-05

def matmul(left, right):
    return jnp.dot(left, right, precision=HIGHEST, preferred_element_type=jnp.float32)

def contract_first(left, right):
    return lax.dot_general(left, right, (((0,), (0,)), ((), ())), precision=HIGHEST, preferred_element_type=jnp.float32)

def layer_norm(values, gain_row, shift_row):
    center = lax.optimization_barrier(jnp.mean(values, axis=1, keepdims=True))
    centred = values - center
    spread = lax.optimization_barrier(jnp.mean(centred * centred, axis=1, keepdims=True))
    return centred * lax.rsqrt(spread + epsilon) * gain_row + shift_row

def edge_section(section_index, send_table, recv_table, feats, senders, receivers, edge_weight, sender_weight, receiver_weight, first_bias, out_weight, out_bias, norm_gain, norm_shift):
    send_terms = matmul(send_table, sender_weight[section_index])
    recv_terms = matmul(recv_table, receiver_weight[section_index])
    patch_total = PLAT * PLON
    slot_count = senders.shape[-1]
    block_feats = feats.reshape(patch_total, feats.shape[2], slot_count)
    block_send = senders.reshape(patch_total, slot_count)
    block_recv = receivers.reshape(patch_total, slot_count)

    def one_patch(bundle):
        place, feat_block, send_ids, recv_ids = bundle
        local_node = jnp.clip(recv_ids - place * M_DEV, 0, M_DEV - 1).astype(jnp.int32)
        global_node = (place * M_DEV + local_node).astype(jnp.int32)
        active = recv_ids >= 0
        hidden = jax.nn.silu(send_terms[send_ids] + recv_terms[global_node] + contract_first(feat_block, edge_weight[section_index]) + first_bias[section_index])
        message = matmul(hidden, out_weight[section_index]) + out_bias[section_index]
        normed = layer_norm(message, norm_gain[section_index], norm_shift[section_index])
        normed = jnp.where(active[:, None], normed, jnp.zeros_like(normed))
        return jax.ops.segment_sum(normed, local_node, num_segments=M_DEV)
    totals = lax.map(one_patch, (jnp.arange(patch_total, dtype=jnp.int32), block_feats, block_send, block_recv))
    return totals.reshape(patch_total * M_DEV, -1)

def reference(grid_latent, mesh_latent, grid_edge_feats, grid_senders, grid_receivers, mesh_edge_feats, mesh_senders, mesh_receivers, edge_weight, sender_weight, receiver_weight, first_bias, out_weight, out_bias, norm_gain, norm_shift):
    weights = (edge_weight, sender_weight, receiver_weight, first_bias, out_weight, out_bias, norm_gain, norm_shift)
    grid_table = grid_latent.reshape(-1, C)
    mesh_table = mesh_latent.reshape(-1, C)
    mesh_mid = mesh_table + edge_section(0, grid_table, mesh_table, grid_edge_feats, grid_senders, grid_receivers, *weights)
    mesh_out = mesh_mid + edge_section(1, mesh_mid, mesh_mid, mesh_edge_feats, mesh_senders, mesh_receivers, *weights)
    return mesh_out.reshape(PLAT, PLON, M_DEV, C)
```

```python
import jax
import jax.numpy as jnp
from jax import lax
from jax.experimental import pallas as pl
from jax.experimental.pallas import tpu as pltpu
from jax.sharding import PartitionSpec as P

RIM = 2
LANES = 128
EDGE_CHUNK = 256
epsilon = 1e-05
F32 = jnp.float32
BF16 = jnp.bfloat16


def split(value):
    high = value.astype(BF16)
    low = (value - high.astype(F32)).astype(BF16)
    return high, low


def dot(left, right):
    return jnp.dot(left, right, preferred_element_type=F32)


def dot_split(left, right):
    left_high, left_low = split(left)
    right_high, right_low = split(right)
    return dot(
        jnp.concatenate([left_high, left_high, left_low], axis=1),
        jnp.concatenate([right_high, right_low, right_high], axis=0),
    )


def down_lanes(index_row):
    return jnp.transpose(jnp.broadcast_to(index_row, (LANES, index_row.shape[1])))


def onehot_rows(index_cols, count):
    lane = lax.broadcasted_iota(jnp.int32, index_cols.shape, 1)
    blocks = [
        jnp.where(index_cols == lane + start, 1.0, 0.0).astype(BF16)
        for start in range(0, count, LANES)
    ]
    return jnp.concatenate(blocks, axis=1)


def pick(index_row, table):
    width = table.shape[1]
    high, low = split(table)
    both = dot(
        onehot_rows(down_lanes(index_row), table.shape[0]), jnp.concatenate([high, low], axis=1)
    )
    return both[:, :width] + both[:, width:]


def edge_terms(feats, weight):
    return lax.dot_general(
        feats,
        weight,
        (((0,), (0,)), ((), ())),
        precision=lax.Precision.HIGHEST,
        preferred_element_type=F32,
    )


def call(body, outs, flops, *args):
    return pl.pallas_call(
        body,
        out_shape=outs,
        cost_estimate=pl.CostEstimate(flops=flops, bytes_accessed=1 << 20, transcendentals=0),
    )(*args)


def shape(*dims):
    return jax.ShapeDtypeStruct(dims, F32)


def exchange(value, axes, move):
    sizes = [lax.axis_size(axis) for axis in axes]
    pairs = []
    total = 1
    for size in sizes:
        total *= size
    for source in range(total):
        rest, target, stride, fits = source, 0, 1, True
        for size, (step, wraps) in list(zip(sizes, move))[::-1]:
            place = rest % size + step
            rest //= size
            if wraps:
                place %= size
            elif not 0 <= place < size:
                fits = False
            target += place * stride
            stride *= size
        if fits:
            pairs.append((source, target))
    return lax.ppermute(value, axes if len(axes) > 1 else axes[0], pairs)


def gather_hid(value):
    count = lax.axis_size("hid")
    pieces = [value]
    for step in range(1, count):
        source, hop = (pieces[step - 1], 1) if step % 2 else (value, step)
        pieces.append(lax.ppermute(source, "hid", [(i, i ^ hop) for i in range(count)]))
    return pieces


def layer_norm(message, gain, shift):
    centred = message - jnp.mean(message, axis=1, keepdims=True)
    spread = jnp.mean(centred * centred, axis=1, keepdims=True)
    return centred * lax.rsqrt(spread + epsilon) * gain + shift


def normed_chunks(hidden_refs, weight_refs, bias_ref, gain_ref, shift_ref, store):
    right = jnp.concatenate([ref[...] for ref in weight_refs], axis=0)
    right_high, right_low = split(right)
    right = jnp.concatenate([right_high, right_low, right_high], axis=0)
    edges = hidden_refs[0].shape[0]
    step = min(EDGE_CHUNK, edges)
    for start in range(0, edges, step):
        left = jnp.concatenate([ref[start : start + step, :] for ref in hidden_refs], axis=1)
        left_high, left_low = split(left)
        left = jnp.concatenate([left_high, left_high, left_low], axis=1)
        message = dot(left, right) + bias_ref[...]
        store(start, step, layer_norm(message, gain_ref[...], shift_ref[...]))


def aggregate(receiver_row, nodes, normed_ref):
    node = lax.broadcasted_iota(jnp.int32, (nodes, receiver_row.shape[1]), 0)
    onehot = jnp.where(node == receiver_row, 1.0, 0.0).astype(BF16)
    width = normed_ref.shape[1] // 2
    both = dot(onehot, normed_ref[...])
    return both[:, :width] + both[:, width:]


def per_device(
    grid_latent,
    mesh_latent,
    grid_edge_feats,
    grid_senders,
    grid_receivers,
    mesh_edge_feats,
    mesh_senders,
    mesh_receivers,
    edge_weight,
    sender_weight,
    receiver_weight,
    first_bias,
    out_weight,
    out_bias,
    norm_gain,
    norm_shift,
):
    lat_index = lax.axis_index("lat")
    lon_index = lax.axis_index("lon")
    lon_count = lax.axis_size("lon")
    hid_index = lax.axis_index("hid")
    hid_count = lax.axis_size("hid")
    rows, cols, width = grid_latent.shape
    nodes = mesh_latent.shape[2]
    units = sender_weight.shape[2]
    grid_edges = grid_senders.shape[2]
    mesh_edges = mesh_senders.shape[2]
    patch = lat_index * lon_count + lon_index
    mesh_own = mesh_latent.reshape(nodes, width)
    cells = grid_latent.reshape(rows * cols, width)
    two_lon = lon_count == 2

    grid_ids = grid_senders.reshape(1, grid_edges)
    total_lon = cols * lon_count
    cell_row = grid_ids // total_lon - lat_index * rows
    cell_col = (grid_ids % total_lon - lon_index * cols + RIM) % total_lon - RIM
    in_rows = (cell_row >= 0) & (cell_row < rows)
    in_cols = (cell_col >= 0) & (cell_col < cols)
    side_slot = jnp.where(cell_col < 0, cell_col + 2 * RIM, cell_col - cols)
    own_cell = jnp.where(in_rows & in_cols, cell_row * cols + cell_col, -1)
    side_size = rows * 2 * RIM
    id_rows = -(-mesh_edges // LANES)
    lat_size = RIM * cols + RIM * 2 * RIM
    lat_pad = -(lat_size + id_rows) % 16
    lat_rows = lat_size + id_rows + lat_pad
    rim_row = jnp.where(cell_row < 0, cell_row + RIM, cell_row - rows)
    rim_place = jnp.where(in_cols, rim_row * cols + cell_col, RIM * cols + rim_row * 2 * RIM + side_slot)
    rim_place = rim_place + side_size + jnp.where(cell_row < 0, 0, lat_rows)
    rim_cell = jnp.where(
        in_rows, jnp.where(in_cols, -1, cell_row * 2 * RIM + side_slot), rim_place
    )
    grid_recv = grid_receivers.reshape(1, grid_edges) - patch * nodes
    mesh_recv = mesh_receivers.reshape(1, mesh_edges) - patch * nodes

    def sender_nodes(ids):
        source = ids // nodes
        here = source // lon_count == lat_index
        offset = (source % lon_count - lon_index) % lon_count
        node = ids % nodes
        tables = [0, 1] if two_lon else [0, lon_count - 1, 1]
        return [jnp.where(here & (offset == place), node, -1) for place in tables]

    mesh_ids = mesh_senders.reshape(1, mesh_edges)
    ids_sent = jnp.pad(
        mesh_ids.reshape(-1).astype(F32), (0, (id_rows + lat_pad) * LANES - mesh_edges)
    ).reshape(id_rows + lat_pad, LANES)

    weight_pieces = gather_hid(out_weight)
    out_weights = [[piece[section] for piece in weight_pieces] for section in range(2)]

    def terms_body(cell_ref, weight_ref, term_ref, side_ref):
        term_ref[...] = dot_split(cell_ref[...], weight_ref[...])
        for row in range(rows):
            start = row * 2 * RIM
            side_ref[start : start + RIM, :] = term_ref[row * cols : row * cols + RIM, :]
            side_ref[start + RIM : start + 2 * RIM, :] = term_ref[
                (row + 1) * cols - RIM : (row + 1) * cols, :
            ]

    terms, sides = call(
        terms_body,
        (shape(rows * cols, units), shape(side_size, units)),
        6 * rows * cols * width * units,
        cells,
        sender_weight[0],
    )
    if two_lon:
        side_got = exchange(sides, ("lon",), ((1, True),))
    else:
        parts = sides.reshape(rows, 2, RIM, units)
        from_high = exchange(parts[:, 0], ("lon",), ((-1, True),))
        from_low = exchange(parts[:, 1], ("lon",), ((1, True),))
        side_got = jnp.stack([from_high, from_low], axis=1).reshape(side_size, units)

    def rim_sent(first):
        return jnp.concatenate(
            [
                terms[first * cols : (first + RIM) * cols],
                side_got[first * 2 * RIM : (first + RIM) * 2 * RIM],
                ids_sent,
            ],
            axis=0,
        )

    rim_low = exchange(rim_sent(rows - RIM), ("lat",), ((1, False),))
    rim_high = exchange(rim_sent(0), ("lat",), ((-1, False),))

    def grid_first_body(term_ref, mesh_ref, weight_ref, feat_ref, edge_ref, bias_ref, send_ref, recv_ref, pre_ref):
        received = dot_split(mesh_ref[...], weight_ref[...])
        pre_ref[...] = (
            pick(send_ref[...], term_ref[...])
            + pick(recv_ref[...], received)
            + edge_terms(feat_ref[...], edge_ref[...])
            + bias_ref[...]
        )

    grid_pre = call(
        grid_first_body,
        shape(grid_edges, units),
        8 * grid_edges * rows * cols * units,
        terms,
        mesh_own,
        receiver_weight[0],
        grid_edge_feats.reshape(-1, grid_edges),
        edge_weight[0],
        first_bias[0:1],
        own_cell,
        grid_recv,
    )

    def grid_hidden_body(pre_ref, side_ref, low_ref, high_ref, send_ref, hidden_ref):
        pad = -(side_size + 2 * lat_rows) % LANES
        table = jnp.concatenate(
            [side_ref[...], low_ref[...], high_ref[...], jnp.zeros((pad, units), F32)], axis=0
        )
        total = pre_ref[...] + pick(send_ref[...], table)
        hidden_ref[...] = total / (1.0 + jnp.exp(-total))

    grid_hidden = call(
        grid_hidden_body,
        shape(grid_edges, units),
        4 * grid_edges * rows * cols * units,
        grid_pre,
        side_got,
        rim_low,
        rim_high,
        rim_cell,
    )
    grid_pieces = gather_hid(grid_hidden)

    def grid_message_body(*refs):
        hidden_refs, weight_refs = refs[:hid_count], refs[hid_count : 2 * hid_count]
        bias_ref, gain_ref, shift_ref, recv_ref, mesh_ref, send_ref = refs[2 * hid_count : -3]
        mid_ref, term_ref, normed_ref = refs[-3:]

        def store(start, step, normed):
            high, low = split(normed)
            normed_ref[start : start + step, :width] = high
            normed_ref[start : start + step, width:] = low

        normed_chunks(hidden_refs, weight_refs, bias_ref, gain_ref, shift_ref, store)
        middle = mesh_ref[...] + aggregate(recv_ref[...], nodes, normed_ref)
        mid_ref[...] = middle
        term_ref[...] = dot_split(middle, send_ref[...])

    mesh_mid, mesh_terms = pl.pallas_call(
        grid_message_body,
        out_shape=(shape(nodes, width), shape(nodes, units)),
        scratch_shapes=[pltpu.VMEM((grid_edges, 2 * width), BF16)],
        cost_estimate=pl.CostEstimate(
            flops=12 * grid_edges * width * width, bytes_accessed=1 << 22, transcendentals=0
        ),
    )(
        *grid_pieces,
        *out_weights[0],
        out_bias[0:1],
        norm_gain[0:1],
        norm_shift[0:1],
        grid_recv,
        mesh_own,
        sender_weight[1],
    )

    if two_lon:
        others = [exchange(mesh_terms, ("lon",), ((1, True),))]
    else:
        others = [
            exchange(mesh_terms, ("lon",), ((1, True),)),
            exchange(mesh_terms, ("lon",), ((-1, True),)),
        ]

    def ids_of(rim):
        return rim[lat_size : lat_size + id_rows].reshape(1, -1)[:, :mesh_edges].astype(jnp.int32)

    own_nodes = sender_nodes(mesh_ids)
    low_nodes = sender_nodes(ids_of(rim_low))
    high_nodes = sender_nodes(ids_of(rim_high))

    def mesh_first_body(term_ref, mid_ref, weight_ref, feat_ref, edge_ref, bias_ref, recv_ref, own_ref, low_ref, high_ref, pre_ref, down_ref, up_ref):
        table = term_ref[...]
        down_ref[...] = pick(low_ref[...], table)
        up_ref[...] = pick(high_ref[...], table)
        received = dot_split(mid_ref[...], weight_ref[...])
        pre_ref[...] = (
            pick(own_ref[...], table)
            + pick(recv_ref[...], received)
            + edge_terms(feat_ref[...], edge_ref[...])
            + bias_ref[...]
        )

    edge_block = shape(mesh_edges, units)
    mesh_pre, down_first, up_first = call(
        mesh_first_body,
        (edge_block, edge_block, edge_block),
        16 * mesh_edges * nodes * units,
        mesh_terms,
        mesh_mid,
        receiver_weight[1],
        mesh_edge_feats.reshape(-1, mesh_edges),
        edge_weight[1],
        first_bias[1:2],
        mesh_recv,
        own_nodes[0],
        low_nodes[0],
        high_nodes[0],
    )

    def add_others(first_ref, index_refs, table_refs):
        total = first_ref[...]
        for index_ref, table_ref in zip(index_refs, table_refs):
            total = total + pick(index_ref[...], table_ref[...])
        return total

    def mesh_sent_body(*refs):
        count = len(others)
        tables = refs[:count]
        refs = refs[count:]
        refs[-2][...] = add_others(refs[0], refs[2 : 2 + count], tables)
        refs[-1][...] = add_others(refs[1], refs[2 + count : 2 + 2 * count], tables)

    down, up = call(
        mesh_sent_body,
        (edge_block, edge_block),
        8 * mesh_edges * nodes * units,
        *others,
        down_first,
        up_first,
        *low_nodes[1:],
        *high_nodes[1:],
    )
    from_high = exchange(down, ("lat",), ((-1, False),))
    from_low = exchange(up, ("lat",), ((1, False),))

    def mesh_own_body(*refs):
        count = len(others)
        refs[-1][...] = add_others(refs[0], refs[1 : 1 + count], refs[1 + count : 1 + 2 * count])

    mesh_pre = call(
        mesh_own_body,
        edge_block,
        4 * mesh_edges * nodes * units,
        mesh_pre,
        *own_nodes[1:],
        *others,
    )

    def mesh_hidden_body(pre_ref, low_ref, high_ref, hidden_ref):
        total = pre_ref[...] + low_ref[...] + high_ref[...]
        hidden_ref[...] = total / (1.0 + jnp.exp(-total))

    mesh_hidden = call(
        mesh_hidden_body, edge_block, mesh_edges * units, mesh_pre, from_low, from_high
    )
    mesh_pieces = gather_hid(mesh_hidden)
    share = width // hid_count

    def mesh_message_body(*refs):
        place_ref = refs[0]
        refs = refs[1:]
        hidden_refs, weight_refs = refs[:hid_count], refs[hid_count : 2 * hid_count]
        bias_ref, gain_ref, shift_ref, recv_ref, mid_ref = refs[2 * hid_count : -2]
        out_ref, normed_ref = refs[-2:]
        place = place_ref[0]

        def own_part(value):
            part = value[:, :share]
            for step in range(1, hid_count):
                part = jnp.where(place == step, value[:, step * share : (step + 1) * share], part)
            return part

        def store(start, step, normed):
            high, low = split(own_part(normed))
            normed_ref[start : start + step, :share] = high
            normed_ref[start : start + step, share:] = low

        normed_chunks(hidden_refs, weight_refs, bias_ref, gain_ref, shift_ref, store)
        out_ref[...] = own_part(mid_ref[...]) + aggregate(recv_ref[...], nodes, normed_ref)

    vmem = pl.BlockSpec(memory_space=pltpu.VMEM)
    mesh_out = pl.pallas_call(
        mesh_message_body,
        out_shape=shape(nodes, share),
        in_specs=[pl.BlockSpec(memory_space=pltpu.SMEM)] + [vmem] * (2 * hid_count + 5),
        out_specs=vmem,
        scratch_shapes=[pltpu.VMEM((mesh_edges, 2 * share), BF16)],
        cost_estimate=pl.CostEstimate(
            flops=8 * mesh_edges * width * width, bytes_accessed=1 << 22, transcendentals=0
        ),
    )(
        hid_index.reshape(1).astype(jnp.int32),
        *mesh_pieces,
        *out_weights[1],
        out_bias[1:2],
        norm_gain[1:2],
        norm_shift[1:2],
        mesh_recv,
        mesh_mid,
    )
    return mesh_out.reshape(1, 1, nodes, share)


def solution(mesh):
    return jax.shard_map(
        per_device,
        mesh=mesh,
        in_specs=(
            P("lat", "lon", None),
            P("lat", "lon", None, None),
            P("lat", "lon", None, None),
            P("lat", "lon", None),
            P("lat", "lon", None),
            P("lat", "lon", None, None),
            P("lat", "lon", None),
            P("lat", "lon", None),
            P(None, None, "hid"),
            P(None, None, "hid"),
            P(None, None, "hid"),
            P(None, "hid"),
            P(None, "hid", None),
            P(),
            P(),
            P(),
        ),
        out_specs=P("lat", "lon", None, "hid"),
        check_vma=False,
    )
```

```python
import jax
import jax.numpy as jnp
from jax import lax
from jax.experimental import pallas as pl
from jax.experimental.pallas import tpu as pltpu
from jax.sharding import PartitionSpec as P

RIM = 2
LANES = 128
EDGE_CHUNK = 256
epsilon = 1e-05
F32 = jnp.float32
BF16 = jnp.bfloat16


def split(value):
    high = value.astype(BF16)
    low = (value - high.astype(F32)).astype(BF16)
    return high, low


def dot(left, right):
    return jnp.dot(left, right, preferred_element_type=F32)


def dot_split(left, right):
    left_high, left_low = split(left)
    right_high, right_low = split(right)
    return dot(
        jnp.concatenate([left_high, left_high, left_low], axis=1),
        jnp.concatenate([right_high, right_low, right_high], axis=0),
    )


def down_lanes(index_row):
    return jnp.transpose(jnp.broadcast_to(index_row, (LANES, index_row.shape[1])))


def onehot_rows(index_cols, count):
    lane = lax.broadcasted_iota(jnp.int32, index_cols.shape, 1)
    blocks = [
        jnp.where(index_cols == lane + start, 1.0, 0.0).astype(BF16)
        for start in range(0, count, LANES)
    ]
    return jnp.concatenate(blocks, axis=1)


def pick(index_row, table):
    width = table.shape[1]
    high, low = split(table)
    both = dot(
        onehot_rows(down_lanes(index_row), table.shape[0]), jnp.concatenate([high, low], axis=1)
    )
    return both[:, :width] + both[:, width:]


def edge_terms(feats, weight):
    return lax.dot_general(
        feats,
        weight,
        (((0,), (0,)), ((), ())),
        precision=lax.Precision.HIGHEST,
        preferred_element_type=F32,
    )


def divide(value, count):
    if count & (count - 1) == 0:
        return value >> (count.bit_length() - 1), value & (count - 1)
    return value // count, value % count


VMEM = pl.BlockSpec(memory_space=pltpu.VMEM)


def call(name, body, outs, flops, args, scratch=()):
    return pl.pallas_call(
        body,
        out_shape=outs,
        in_specs=[VMEM] * len(args),
        out_specs=jax.tree.map(lambda _: VMEM, outs),
        scratch_shapes=scratch,
        name=name,
        cost_estimate=pl.CostEstimate(flops=flops, bytes_accessed=1 << 20, transcendentals=0),
    )(*args)


def shape(*dims, dtype=F32):
    return jax.ShapeDtypeStruct(dims, dtype)


def shift(value, axis, step):
    count = lax.axis_size(axis)
    return lax.ppermute(value, axis, [(i, (i + step) % count) for i in range(count)])


def swap_lat(value, first):
    count = lax.axis_size("lat")
    pairs = [(i, i + 1) for i in range(first, count - 1, 2)]
    return lax.ppermute(value, "lat", pairs + [(high, low) for low, high in pairs])


def gather_hid(value):
    count = lax.axis_size("hid")
    pieces = [value]
    for step in range(1, count):
        source, hop = (pieces[step - 1], 1) if step % 2 else (value, step)
        pieces.append(lax.ppermute(source, "hid", [(i, i ^ hop) for i in range(count)]))
    return pieces


def layer_norm(message, gain, shift):
    centred = message - jnp.mean(message, axis=1, keepdims=True)
    spread = jnp.mean(centred * centred, axis=1, keepdims=True)
    return centred * lax.rsqrt(spread + epsilon) * gain + shift


def normed_chunks(hidden_refs, weight_ref, bias, gain, shift_row, store):
    edges = hidden_refs[0].shape[0]
    step = min(EDGE_CHUNK, edges)
    for start in range(0, edges, step):
        left = jnp.concatenate([ref[start : start + step, :] for ref in hidden_refs], axis=1)
        left_high, left_low = split(left)
        left = jnp.concatenate([left_high, left_high, left_low], axis=1)
        message = dot(left, weight_ref[...]) + bias
        store(start, step, layer_norm(message, gain, shift_row))


def aggregate(receiver_row, nodes, normed_ref):
    node = lax.broadcasted_iota(jnp.int32, (nodes, receiver_row.shape[1]), 0)
    onehot = jnp.where(node == receiver_row, 1.0, 0.0).astype(BF16)
    width = normed_ref.shape[1] // 2
    both = dot(onehot, normed_ref[...])
    return both[:, :width] + both[:, width:]


def per_device(
    grid_latent,
    mesh_latent,
    grid_edge_feats,
    grid_senders,
    grid_receivers,
    mesh_edge_feats,
    mesh_senders,
    mesh_receivers,
    edge_weight,
    sender_weight,
    receiver_weight,
    first_bias,
    out_weight,
    out_bias,
    norm_gain,
    norm_shift,
):
    lon_count = lax.axis_size("lon")
    hid_count = lax.axis_size("hid")
    rows, cols, width = grid_latent.shape
    nodes = mesh_latent.shape[2]
    units = sender_weight.shape[2]
    grid_edges = grid_senders.shape[2]
    mesh_edges = mesh_senders.shape[2]
    mesh_own = mesh_latent.reshape(nodes, width)
    cells = grid_latent.reshape(rows * cols, width)
    grid_ids = grid_senders.reshape(1, grid_edges)
    grid_to = grid_receivers.reshape(1, grid_edges)
    mesh_ids = mesh_senders.reshape(1, mesh_edges)
    mesh_to = mesh_receivers.reshape(1, mesh_edges)
    two_lon = lon_count == 2
    side_size = rows * 2 * RIM
    id_rows = mesh_edges // LANES
    lat_size = RIM * cols + RIM * 2 * RIM
    lat_rows = lat_size + id_rows + -(lat_size + id_rows) % 16

    def local(receivers):
        patch = lax.axis_index("lat") * lon_count + lax.axis_index("lon")
        return receivers - patch * nodes

    def cell_places(ids):
        lat_index = lax.axis_index("lat")
        total_lon = cols * lon_count
        row, col = divide(ids, total_lon)
        row = row - lat_index * rows
        col = divide(col - lax.axis_index("lon") * cols + RIM, total_lon)[1] - RIM
        in_rows = (row >= 0) & (row < rows)
        in_cols = (col >= 0) & (col < cols)
        own = jnp.where(in_rows & in_cols, row * cols + col, -1)
        slot = jnp.where(col < 0, col + 2 * RIM, col - cols)
        rim_row = jnp.where(row < 0, row + RIM, row - rows)
        rim = jnp.where(in_cols, rim_row * cols + col, RIM * cols + rim_row * 2 * RIM + slot)
        odd = lat_index % 2
        rim = rim + side_size + jnp.where(row < 0, 1 - odd, odd) * lat_rows
        beyond = jnp.where(in_rows, jnp.where(in_cols, -1, row * 2 * RIM + slot), rim)
        return own, beyond

    def sender_nodes(ids):
        source, node = divide(ids, nodes)
        source_lat, source_lon = divide(source, lon_count)
        here = source_lat == lax.axis_index("lat")
        offset = divide(source_lon - lax.axis_index("lon") + lon_count, lon_count)[1]
        tables = [0, 1] if two_lon else [0, lon_count - 1, 1]
        return [jnp.where(here & (offset == place), node, -1) for place in tables]

    def ids_in(rim_ref):
        rim_ids = [rim_ref[lat_size + row : lat_size + row + 1, :] for row in range(id_rows)]
        return jnp.concatenate(rim_ids, axis=1).astype(jnp.int32)

    step_rows = 2 if rows % 2 == 0 else 1

    def terms_body(cell_ref, weight_ref, term_ref, side_ref):
        term_ref[...] = dot_split(cell_ref[...], weight_ref[...])
        for row in range(step_rows):
            start = row * 2 * RIM
            side_ref[start : start + RIM, :] = term_ref[row * cols : row * cols + RIM, :]
            side_ref[start + RIM : start + 2 * RIM, :] = term_ref[
                (row + 1) * cols - RIM : (row + 1) * cols, :
            ]

    terms, sides = pl.pallas_call(
        terms_body,
        grid=(rows // step_rows,),
        in_specs=[
            pl.BlockSpec((step_rows * cols, width), lambda i: (i, 0)),
            pl.BlockSpec((None, width, units), lambda i: (0, 0, 0)),
        ],
        out_shape=(shape(rows * cols, units), shape(side_size, units)),
        out_specs=(
            pl.BlockSpec((step_rows * cols, units), lambda i: (i, 0)),
            pl.BlockSpec((step_rows * 2 * RIM, units), lambda i: (i, 0)),
        ),
        name="grid_terms",
        cost_estimate=pl.CostEstimate(
            flops=6 * rows * cols * width * units, bytes_accessed=1 << 21, transcendentals=0
        ),
    )(cells, sender_weight)
    if two_lon:
        side_got = shift(sides, "lon", 1)
    else:
        parts = sides.reshape(rows, 2, RIM, units)
        from_high = shift(parts[:, 0], "lon", -1)
        from_low = shift(parts[:, 1], "lon", 1)
        side_got = jnp.stack([from_high, from_low], axis=1).reshape(side_size, units)

    out_pieces = gather_hid(lax.optimization_barrier((out_weight, sides))[0])

    def grid_received_body(mesh_ref, weight_ref, feat_ref, edge_ref, bias_ref, recv_ref, pre_ref):
        received = dot_split(mesh_ref[...], weight_ref[0])
        pre_ref[...] = (
            pick(local(recv_ref[...]), received)
            + edge_terms(feat_ref[...], edge_ref[0])
            + bias_ref[0:1, :]
        )

    grid_pre = call(
        "grid_received",
        grid_received_body,
        shape(grid_edges, units),
        8 * grid_edges * rows * cols * units,
        (mesh_own, receiver_weight, grid_edge_feats.reshape(-1, grid_edges), edge_weight, first_bias, grid_to),
    )

    def rim_body(term_ref, side_ref, id_ref, a_ref, b_ref):
        odd = lax.axis_index("lat") % 2
        for ref, up in ((a_ref, 1 - odd), (b_ref, odd)):
            start = up * (rows - RIM)
            ref[: RIM * cols, :] = term_ref[pl.ds(pl.multiple_of(start * cols, 8), RIM * cols), :]
            ref[RIM * cols : lat_size, :] = jnp.where(
                up == 1,
                side_ref[(rows - RIM) * 2 * RIM : rows * 2 * RIM, :],
                side_ref[: RIM * 2 * RIM, :],
            )
            ids = id_ref[...].astype(F32)
            for row in range(id_rows):
                ref[lat_size + row : lat_size + row + 1, :] = ids[:, row * LANES : (row + 1) * LANES]
            ref[lat_size + id_rows :, :] = jnp.zeros((lat_rows - lat_size - id_rows, units), F32)

    rim_block = shape(lat_rows, units)
    rim_a, rim_b = call(
        "grid_rim", rim_body, (rim_block, rim_block), 1 << 20, (terms, side_got, mesh_ids)
    )
    rim_a = swap_lat(rim_a, 0)
    rim_b = swap_lat(rim_b, 1)

    def grid_own_body(pre_ref, term_ref, send_ref, out_ref):
        out_ref[...] = pre_ref[...] + pick(cell_places(send_ref[...])[0], term_ref[...])

    grid_pre = call(
        "grid_own",
        grid_own_body,
        shape(grid_edges, units),
        8 * grid_edges * rows * cols * units,
        (grid_pre, terms, grid_ids),
    )

    def grid_hidden_body(pre_ref, side_ref, a_ref, b_ref, send_ref, hidden_ref):
        pad = -(side_size + 2 * lat_rows) % LANES
        table = jnp.concatenate(
            [side_ref[...], a_ref[...], b_ref[...], jnp.zeros((pad, units), F32)], axis=0
        )
        total = pre_ref[...] + pick(cell_places(send_ref[...])[1], table)
        hidden_ref[...] = total / (1.0 + jnp.exp(-total))

    grid_hidden = call(
        "grid_hidden",
        grid_hidden_body,
        shape(grid_edges, units),
        4 * grid_edges * rows * cols * units,
        (grid_pre, side_got, rim_a, rim_b, grid_ids),
    )
    grid_pieces = gather_hid(grid_hidden)

    def weight_body(*refs):
        for section in range(2):
            whole = jnp.concatenate([ref[section] for ref in refs[:hid_count]], axis=0)
            high, low = split(whole)
            out_ref = refs[hid_count + section]
            out_ref[:width, :] = high
            out_ref[width : 2 * width, :] = low
            out_ref[2 * width :, :] = high

    weight_block = shape(3 * width, width, dtype=BF16)
    whole_weights = call(
        "weights",
        weight_body,
        (weight_block, weight_block),
        1 << 30,
        lax.optimization_barrier((*out_pieces, grid_hidden))[:hid_count],
    )

    def grid_message_body(*refs):
        hidden_refs = refs[:hid_count]
        weight_ref, bias_ref, gain_ref, shift_ref, recv_ref, mesh_ref, send_ref = refs[hid_count:-3]
        mid_ref, term_ref, normed_ref = refs[-3:]

        def store(start, step, normed):
            high, low = split(normed)
            normed_ref[start : start + step, :width] = high
            normed_ref[start : start + step, width:] = low

        normed_chunks(
            hidden_refs, weight_ref, bias_ref[0:1, :], gain_ref[0:1, :], shift_ref[0:1, :], store
        )
        middle = mesh_ref[...] + aggregate(local(recv_ref[...]), nodes, normed_ref)
        mid_ref[...] = middle
        term_ref[...] = dot_split(middle, send_ref[1])

    mesh_mid, mesh_terms = call(
        "grid_message",
        grid_message_body,
        (shape(nodes, width), shape(nodes, units)),
        12 * grid_edges * width * width,
        (*grid_pieces, whole_weights[0], out_bias, norm_gain, norm_shift, grid_to, mesh_own, sender_weight),
        (pltpu.VMEM((grid_edges, 2 * width), BF16),),
    )

    others = [shift(mesh_terms, "lon", 1)]
    if not two_lon:
        others.append(shift(mesh_terms, "lon", -1))
    table_count = len(others)

    def mesh_first_body(
        term_ref, mid_ref, weight_ref, feat_ref, edge_ref, bias_ref, recv_ref, id_ref, rim_a_ref, rim_b_ref,
        pre_ref, a_ref, b_ref,
    ):
        table = term_ref[...]
        a_ref[...] = pick(sender_nodes(ids_in(rim_a_ref))[0], table)
        b_ref[...] = pick(sender_nodes(ids_in(rim_b_ref))[0], table)
        received = dot_split(mid_ref[...], weight_ref[1])
        pre_ref[...] = (
            pick(sender_nodes(id_ref[...])[0], table)
            + pick(local(recv_ref[...]), received)
            + edge_terms(feat_ref[...], edge_ref[1])
            + bias_ref[1:2, :]
        )

    edge_block = shape(mesh_edges, units)
    mesh_pre, send_a, send_b = call(
        "mesh_first",
        mesh_first_body,
        (edge_block, edge_block, edge_block),
        16 * mesh_edges * nodes * units,
        (
            mesh_terms, mesh_mid, receiver_weight, mesh_edge_feats.reshape(-1, mesh_edges), edge_weight,
            first_bias, mesh_to, mesh_ids, rim_a, rim_b,
        ),
    )

    def add_others(first_ref, ids, table_refs):
        total = first_ref[...]
        for index_row, table_ref in zip(sender_nodes(ids)[1:], table_refs):
            total = total + pick(index_row, table_ref[...])
        return total

    def mesh_sent_body(*refs):
        tables = refs[:table_count]
        first_a, first_b, rim_a_ref, rim_b_ref, a_ref, b_ref = refs[table_count:]
        a_ref[...] = add_others(first_a, ids_in(rim_a_ref), tables)
        b_ref[...] = add_others(first_b, ids_in(rim_b_ref), tables)

    send_a, send_b = call(
        "mesh_sent",
        mesh_sent_body,
        (edge_block, edge_block),
        8 * mesh_edges * nodes * units,
        (*others, send_a, send_b, rim_a, rim_b),
    )
    got_a = swap_lat(send_a, 0)
    got_b = swap_lat(send_b, 1)

    def mesh_own_body(*refs):
        first_ref, id_ref, out_ref = refs[table_count:]
        out_ref[...] = add_others(first_ref, id_ref[...], refs[:table_count])

    mesh_pre = call(
        "mesh_own",
        mesh_own_body,
        edge_block,
        4 * mesh_edges * nodes * units,
        (*others, mesh_pre, mesh_ids),
    )
    total = mesh_pre + got_a + got_b
    mesh_pieces = gather_hid(total / (1.0 + jnp.exp(-total)))
    share = width // hid_count

    def mesh_message_body(*refs):
        hidden_refs = refs[:hid_count]
        weight_ref, bias_ref, gain_ref, shift_ref, recv_ref, mid_ref, out_ref, normed_ref = refs[hid_count:]
        place = lax.axis_index("hid")

        def own_part(value):
            part = value[:, :share]
            for step in range(1, hid_count):
                part = jnp.where(place == step, value[:, step * share : (step + 1) * share], part)
            return part

        def store(start, step, normed):
            high, low = split(own_part(normed))
            normed_ref[start : start + step, :share] = high
            normed_ref[start : start + step, share:] = low

        normed_chunks(
            hidden_refs, weight_ref, bias_ref[1:2, :], gain_ref[1:2, :], shift_ref[1:2, :], store
        )
        out_ref[...] = own_part(mid_ref[...]) + aggregate(local(recv_ref[...]), nodes, normed_ref)

    mesh_out = call(
        "mesh_message",
        mesh_message_body,
        shape(nodes, share),
        8 * mesh_edges * width * width,
        (*mesh_pieces, whole_weights[1], out_bias, norm_gain, norm_shift, mesh_to, mesh_mid),
        (pltpu.VMEM((mesh_edges, 2 * share), BF16),),
    )
    return mesh_out.reshape(1, 1, nodes, share)


def solution(mesh):
    return jax.shard_map(
        per_device,
        mesh=mesh,
        in_specs=(
            P("lat", "lon", None),
            P("lat", "lon", None, None),
            P("lat", "lon", None, None),
            P("lat", "lon", None),
            P("lat", "lon", None),
            P("lat", "lon", None, None),
            P("lat", "lon", None),
            P("lat", "lon", None),
            P(None, None, "hid"),
            P(None, None, "hid"),
            P(None, None, "hid"),
            P(None, "hid"),
            P(None, "hid", None),
            P(),
            P(),
            P(),
        ),
        out_specs=P("lat", "lon", None, "hid"),
        check_vma=False,
    )
```

```python
import jax
import jax.numpy as jnp
from jax import lax
from jax.experimental import pallas as pl
from jax.experimental.pallas import tpu as pltpu
from jax.sharding import PartitionSpec as P

RIM = 2
LANES = 128
EDGE_CHUNK = 256
KERNEL_VMEM = 24 << 20
epsilon = 1e-05
F32 = jnp.float32
BF16 = jnp.bfloat16


def split(value):
    high = value.astype(BF16)
    low = (value - high.astype(F32)).astype(BF16)
    return high, low


def dot(left, right):
    return jnp.dot(left, right, preferred_element_type=F32)


def dot_split(left, right):
    left_high, left_low = split(left)
    right_high, right_low = split(right)
    return dot(
        jnp.concatenate([left_high, left_high, left_low], axis=1),
        jnp.concatenate([right_high, right_low, right_high], axis=0),
    )


def down_lanes(index_row):
    return jnp.transpose(jnp.broadcast_to(index_row, (LANES, index_row.shape[1])))


def onehot_rows(index_cols, count):
    lane = lax.broadcasted_iota(jnp.int32, index_cols.shape, 1)
    blocks = [
        jnp.where(index_cols == lane + start, 1.0, 0.0).astype(BF16)
        for start in range(0, count, LANES)
    ]
    return jnp.concatenate(blocks, axis=1)


def pick(index_row, table):
    width = table.shape[1]
    high, low = split(table)
    both = dot(
        onehot_rows(down_lanes(index_row), table.shape[0]), jnp.concatenate([high, low], axis=1)
    )
    return both[:, :width] + both[:, width:]


def edge_terms(feats, weight):
    return lax.dot_general(
        feats,
        weight,
        (((0,), (0,)), ((), ())),
        precision=lax.Precision.HIGHEST,
        preferred_element_type=F32,
    )


def divide(value, count):
    if count & (count - 1) == 0:
        return value >> (count.bit_length() - 1), value & (count - 1)
    return value // count, value % count


VMEM = pl.BlockSpec(memory_space=pltpu.VMEM)


def call(name, body, outs, flops, args, scratch=()):
    return pl.pallas_call(
        body,
        out_shape=outs,
        in_specs=[VMEM] * len(args),
        out_specs=jax.tree.map(lambda _: VMEM, outs),
        scratch_shapes=scratch,
        name=name,
        compiler_params=pltpu.CompilerParams(vmem_limit_bytes=KERNEL_VMEM),
        cost_estimate=pl.CostEstimate(flops=flops, bytes_accessed=1 << 20, transcendentals=0),
    )(*args)


def shape(*dims, dtype=F32):
    return jax.ShapeDtypeStruct(dims, dtype)


def shift(value, axis, step):
    count = lax.axis_size(axis)
    return lax.ppermute(value, axis, [(i, (i + step) % count) for i in range(count)])


def swap_lat(value, first):
    count = lax.axis_size("lat")
    pairs = [(i, i + 1) for i in range(first, count - 1, 2)]
    return lax.ppermute(value, "lat", pairs + [(high, low) for low, high in pairs])


def gather_hid(value):
    count = lax.axis_size("hid")
    pieces = [value]
    for step in range(1, count):
        source, hop = (pieces[step - 1], 1) if step % 2 else (value, step)
        pieces.append(lax.ppermute(source, "hid", [(i, i ^ hop) for i in range(count)]))
    return pieces


def layer_norm(message, gain, shift):
    centred = message - jnp.mean(message, axis=1, keepdims=True)
    spread = jnp.mean(centred * centred, axis=1, keepdims=True)
    return centred * lax.rsqrt(spread + epsilon) * gain + shift


def normed_chunks(hidden_refs, weight_ref, bias, gain, shift_row, store):
    edges = hidden_refs[0].shape[0]
    step = min(EDGE_CHUNK, edges)
    for start in range(0, edges, step):
        left = jnp.concatenate([ref[start : start + step, :] for ref in hidden_refs], axis=1)
        left_high, left_low = split(left)
        left = jnp.concatenate([left_high, left_high, left_low], axis=1)
        message = dot(left, weight_ref[...]) + bias
        store(start, step, layer_norm(message, gain, shift_row))


def aggregate(receiver_row, nodes, normed_ref):
    node = lax.broadcasted_iota(jnp.int32, (nodes, receiver_row.shape[1]), 0)
    onehot = jnp.where(node == receiver_row, 1.0, 0.0).astype(BF16)
    width = normed_ref.shape[1] // 2
    both = dot(onehot, normed_ref[...])
    return both[:, :width] + both[:, width:]


def per_device(
    grid_latent,
    mesh_latent,
    grid_edge_feats,
    grid_senders,
    grid_receivers,
    mesh_edge_feats,
    mesh_senders,
    mesh_receivers,
    edge_weight,
    sender_weight,
    receiver_weight,
    first_bias,
    out_weight,
    out_bias,
    norm_gain,
    norm_shift,
):
    lon_count = lax.axis_size("lon")
    hid_count = lax.axis_size("hid")
    rows, cols, width = grid_latent.shape
    nodes = mesh_latent.shape[2]
    units = sender_weight.shape[2]
    grid_edges = grid_senders.shape[2]
    mesh_edges = mesh_senders.shape[2]
    mesh_own = mesh_latent.reshape(nodes, width)
    cells = grid_latent.reshape(rows * cols, width)
    grid_ids = grid_senders.reshape(1, grid_edges)
    grid_to = grid_receivers.reshape(1, grid_edges)
    mesh_ids = mesh_senders.reshape(1, mesh_edges)
    mesh_to = mesh_receivers.reshape(1, mesh_edges)
    two_lon = lon_count == 2
    side_size = rows * 2 * RIM
    id_rows = mesh_edges // LANES
    lat_size = RIM * cols + RIM * 2 * RIM
    lat_rows = lat_size + id_rows + -(lat_size + id_rows) % 16

    def local(receivers):
        patch = lax.axis_index("lat") * lon_count + lax.axis_index("lon")
        return receivers - patch * nodes

    def cell_places(ids):
        lat_index = lax.axis_index("lat")
        total_lon = cols * lon_count
        row, col = divide(ids, total_lon)
        row = row - lat_index * rows
        col = divide(col - lax.axis_index("lon") * cols + RIM, total_lon)[1] - RIM
        in_rows = (row >= 0) & (row < rows)
        in_cols = (col >= 0) & (col < cols)
        own = jnp.where(in_rows & in_cols, row * cols + col, -1)
        slot = jnp.where(col < 0, col + 2 * RIM, col - cols)
        rim_row = jnp.where(row < 0, row + RIM, row - rows)
        rim = jnp.where(in_cols, rim_row * cols + col, RIM * cols + rim_row * 2 * RIM + slot)
        odd = lat_index % 2
        rim = rim + side_size + jnp.where(row < 0, 1 - odd, odd) * lat_rows
        beyond = jnp.where(in_rows, jnp.where(in_cols, -1, row * 2 * RIM + slot), rim)
        return own, beyond

    def sender_nodes(ids):
        source, node = divide(ids, nodes)
        source_lat, source_lon = divide(source, lon_count)
        here = source_lat == lax.axis_index("lat")
        offset = divide(source_lon - lax.axis_index("lon") + lon_count, lon_count)[1]
        tables = [0, 1] if two_lon else [0, lon_count - 1, 1]
        return [jnp.where(here & (offset == place), node, -1) for place in tables]

    def ids_in(rim_ref):
        rim_ids = [rim_ref[lat_size + row : lat_size + row + 1, :] for row in range(id_rows)]
        return jnp.concatenate(rim_ids, axis=1).astype(jnp.int32)

    step_rows = 2 if rows % 2 == 0 else 1

    def terms_body(cell_ref, weight_ref, term_ref, side_ref):
        term_ref[...] = dot_split(cell_ref[...], weight_ref[...])
        for row in range(step_rows):
            start = row * 2 * RIM
            side_ref[start : start + RIM, :] = term_ref[row * cols : row * cols + RIM, :]
            side_ref[start + RIM : start + 2 * RIM, :] = term_ref[
                (row + 1) * cols - RIM : (row + 1) * cols, :
            ]

    terms, sides = pl.pallas_call(
        terms_body,
        grid=(rows // step_rows,),
        in_specs=[
            pl.BlockSpec((step_rows * cols, width), lambda i: (i, 0)),
            pl.BlockSpec((None, width, units), lambda i: (0, 0, 0)),
        ],
        out_shape=(shape(rows * cols, units), shape(side_size, units)),
        out_specs=(
            pl.BlockSpec((step_rows * cols, units), lambda i: (i, 0)),
            pl.BlockSpec((step_rows * 2 * RIM, units), lambda i: (i, 0)),
        ),
        name="grid_terms",
        compiler_params=pltpu.CompilerParams(vmem_limit_bytes=KERNEL_VMEM),
        cost_estimate=pl.CostEstimate(
            flops=6 * rows * cols * width * units, bytes_accessed=1 << 21, transcendentals=0
        ),
    )(cells, sender_weight)
    if two_lon:
        side_got = shift(sides, "lon", 1)
    else:
        parts = sides.reshape(rows, 2, RIM, units)
        from_high = shift(parts[:, 0], "lon", -1)
        from_low = shift(parts[:, 1], "lon", 1)
        side_got = jnp.stack([from_high, from_low], axis=1).reshape(side_size, units)

    out_pieces = gather_hid(lax.optimization_barrier((out_weight, sides))[0])

    def grid_received_body(mesh_ref, weight_ref, feat_ref, edge_ref, bias_ref, recv_ref, pre_ref):
        received = dot_split(mesh_ref[...], weight_ref[0])
        pre_ref[...] = (
            pick(local(recv_ref[...]), received)
            + edge_terms(feat_ref[...], edge_ref[0])
            + bias_ref[0:1, :]
        )

    grid_pre = call(
        "grid_received",
        grid_received_body,
        shape(grid_edges, units),
        8 * grid_edges * rows * cols * units,
        (mesh_own, receiver_weight, grid_edge_feats.reshape(-1, grid_edges), edge_weight, first_bias, grid_to),
    )

    def rim_body(term_ref, side_ref, id_ref, a_ref, b_ref):
        odd = lax.axis_index("lat") % 2
        for ref, up in ((a_ref, 1 - odd), (b_ref, odd)):
            start = up * (rows - RIM)
            ref[: RIM * cols, :] = term_ref[pl.ds(pl.multiple_of(start * cols, 8), RIM * cols), :]
            ref[RIM * cols : lat_size, :] = jnp.where(
                up == 1,
                side_ref[(rows - RIM) * 2 * RIM : rows * 2 * RIM, :],
                side_ref[: RIM * 2 * RIM, :],
            )
            ids = id_ref[...].astype(F32)
            for row in range(id_rows):
                ref[lat_size + row : lat_size + row + 1, :] = ids[:, row * LANES : (row + 1) * LANES]
            ref[lat_size + id_rows :, :] = jnp.zeros((lat_rows - lat_size - id_rows, units), F32)

    rim_block = shape(lat_rows, units)
    rim_a, rim_b = call(
        "grid_rim", rim_body, (rim_block, rim_block), 1 << 20, (terms, side_got, mesh_ids)
    )
    rim_a = swap_lat(rim_a, 0)
    rim_b = swap_lat(rim_b, 1)

    def grid_own_body(pre_ref, term_ref, send_ref, out_ref):
        out_ref[...] = pre_ref[...] + pick(cell_places(send_ref[...])[0], term_ref[...])

    grid_pre = call(
        "grid_own",
        grid_own_body,
        shape(grid_edges, units),
        8 * grid_edges * rows * cols * units,
        (grid_pre, terms, grid_ids),
    )

    def grid_hidden_body(pre_ref, side_ref, a_ref, b_ref, send_ref, hidden_ref):
        pad = -(side_size + 2 * lat_rows) % LANES
        table = jnp.concatenate(
            [side_ref[...], a_ref[...], b_ref[...], jnp.zeros((pad, units), F32)], axis=0
        )
        total = pre_ref[...] + pick(cell_places(send_ref[...])[1], table)
        hidden_ref[...] = total / (1.0 + jnp.exp(-total))

    grid_hidden = call(
        "grid_hidden",
        grid_hidden_body,
        shape(grid_edges, units),
        4 * grid_edges * rows * cols * units,
        (grid_pre, side_got, rim_a, rim_b, grid_ids),
    )
    grid_pieces = gather_hid(grid_hidden)

    def weight_body(*refs):
        for section in range(2):
            whole = jnp.concatenate([ref[section] for ref in refs[:hid_count]], axis=0)
            high, low = split(whole)
            out_ref = refs[hid_count + section]
            out_ref[:width, :] = high
            out_ref[width : 2 * width, :] = low
            out_ref[2 * width :, :] = high

    weight_block = shape(3 * width, width, dtype=BF16)
    whole_weights = call(
        "weights",
        weight_body,
        (weight_block, weight_block),
        1 << 30,
        lax.optimization_barrier((*out_pieces, grid_hidden))[:hid_count],
    )

    def grid_message_body(*refs):
        hidden_refs = refs[:hid_count]
        weight_ref, bias_ref, gain_ref, shift_ref, recv_ref, mesh_ref, send_ref = refs[hid_count:-3]
        mid_ref, term_ref, normed_ref = refs[-3:]

        def store(start, step, normed):
            high, low = split(normed)
            normed_ref[start : start + step, :width] = high
            normed_ref[start : start + step, width:] = low

        normed_chunks(
            hidden_refs, weight_ref, bias_ref[0:1, :], gain_ref[0:1, :], shift_ref[0:1, :], store
        )
        middle = mesh_ref[...] + aggregate(local(recv_ref[...]), nodes, normed_ref)
        mid_ref[...] = middle
        term_ref[...] = dot_split(middle, send_ref[1])

    mesh_mid, mesh_terms = call(
        "grid_message",
        grid_message_body,
        (shape(nodes, width), shape(nodes, units)),
        12 * grid_edges * width * width,
        (*grid_pieces, whole_weights[0], out_bias, norm_gain, norm_shift, grid_to, mesh_own, sender_weight),
        (pltpu.VMEM((grid_edges, 2 * width), BF16),),
    )

    others = [shift(mesh_terms, "lon", 1)]
    if not two_lon:
        others.append(shift(mesh_terms, "lon", -1))
    table_count = len(others)

    def mesh_first_body(
        term_ref, mid_ref, weight_ref, feat_ref, edge_ref, bias_ref, recv_ref, id_ref, rim_a_ref, rim_b_ref,
        pre_ref, a_ref, b_ref,
    ):
        table = term_ref[...]
        a_ref[...] = pick(sender_nodes(ids_in(rim_a_ref))[0], table)
        b_ref[...] = pick(sender_nodes(ids_in(rim_b_ref))[0], table)
        received = dot_split(mid_ref[...], weight_ref[1])
        pre_ref[...] = (
            pick(sender_nodes(id_ref[...])[0], table)
            + pick(local(recv_ref[...]), received)
            + edge_terms(feat_ref[...], edge_ref[1])
            + bias_ref[1:2, :]
        )

    edge_block = shape(mesh_edges, units)
    mesh_pre, send_a, send_b = call(
        "mesh_first",
        mesh_first_body,
        (edge_block, edge_block, edge_block),
        16 * mesh_edges * nodes * units,
        (
            mesh_terms, mesh_mid, receiver_weight, mesh_edge_feats.reshape(-1, mesh_edges), edge_weight,
            first_bias, mesh_to, mesh_ids, rim_a, rim_b,
        ),
    )

    def add_others(first_ref, ids, table_refs):
        total = first_ref[...]
        for index_row, table_ref in zip(sender_nodes(ids)[1:], table_refs):
            total = total + pick(index_row, table_ref[...])
        return total

    def mesh_sent_body(*refs):
        tables = refs[:table_count]
        first_a, first_b, rim_a_ref, rim_b_ref, a_ref, b_ref = refs[table_count:]
        a_ref[...] = add_others(first_a, ids_in(rim_a_ref), tables)
        b_ref[...] = add_others(first_b, ids_in(rim_b_ref), tables)

    send_a, send_b = call(
        "mesh_sent",
        mesh_sent_body,
        (edge_block, edge_block),
        8 * mesh_edges * nodes * units,
        (*others, send_a, send_b, rim_a, rim_b),
    )
    got_a = swap_lat(send_a, 0)
    got_b = swap_lat(send_b, 1)

    def mesh_own_body(*refs):
        first_ref, id_ref, out_ref = refs[table_count:]
        out_ref[...] = add_others(first_ref, id_ref[...], refs[:table_count])

    mesh_pre = call(
        "mesh_own",
        mesh_own_body,
        edge_block,
        4 * mesh_edges * nodes * units,
        (*others, mesh_pre, mesh_ids),
    )
    total = mesh_pre + got_a + got_b
    mesh_pieces = gather_hid(total / (1.0 + jnp.exp(-total)))
    share = width // hid_count

    def mesh_message_body(*refs):
        hidden_refs = refs[:hid_count]
        weight_ref, bias_ref, gain_ref, shift_ref, recv_ref, mid_ref, out_ref, normed_ref = refs[hid_count:]
        place = lax.axis_index("hid")

        def own_part(value):
            part = value[:, :share]
            for step in range(1, hid_count):
                part = jnp.where(place == step, value[:, step * share : (step + 1) * share], part)
            return part

        def store(start, step, normed):
            high, low = split(own_part(normed))
            normed_ref[start : start + step, :share] = high
            normed_ref[start : start + step, share:] = low

        normed_chunks(
            hidden_refs, weight_ref, bias_ref[1:2, :], gain_ref[1:2, :], shift_ref[1:2, :], store
        )
        out_ref[...] = own_part(mid_ref[...]) + aggregate(local(recv_ref[...]), nodes, normed_ref)

    mesh_out = call(
        "mesh_message",
        mesh_message_body,
        shape(nodes, share),
        8 * mesh_edges * width * width,
        (*mesh_pieces, whole_weights[1], out_bias, norm_gain, norm_shift, mesh_to, mesh_mid),
        (pltpu.VMEM((mesh_edges, 2 * share), BF16),),
    )
    return mesh_out.reshape(1, 1, nodes, share)


def solution(mesh):
    return jax.shard_map(
        per_device,
        mesh=mesh,
        in_specs=(
            P("lat", "lon", None),
            P("lat", "lon", None, None),
            P("lat", "lon", None, None),
            P("lat", "lon", None),
            P("lat", "lon", None),
            P("lat", "lon", None, None),
            P("lat", "lon", None),
            P("lat", "lon", None),
            P(None, None, "hid"),
            P(None, None, "hid"),
            P(None, None, "hid"),
            P(None, "hid"),
            P(None, "hid", None),
            P(),
            P(),
            P(),
        ),
        out_specs=P("lat", "lon", None, "hid"),
        check_vma=False,
    )
```

```python
import jax
import jax.numpy as jnp
from jax import lax
from jax.experimental import pallas as pl
from jax.experimental.pallas import tpu as pltpu
from jax.sharding import PartitionSpec as P

RIM = 2
LANES = 128
EDGE_CHUNK = 256
KERNEL_VMEM = 24 << 20
epsilon = 1e-05
F32 = jnp.float32
BF16 = jnp.bfloat16


def split(value):
    high = value.astype(BF16)
    low = (value - high.astype(F32)).astype(BF16)
    return high, low


def dot(left, right):
    return jnp.dot(left, right, preferred_element_type=F32)


def dot_split(left, right):
    left_high, left_low = split(left)
    right_high, right_low = split(right)
    return dot(
        jnp.concatenate([left_high, left_high, left_low], axis=1),
        jnp.concatenate([right_high, right_low, right_high], axis=0),
    )


def down_lanes(index_row):
    return jnp.transpose(jnp.broadcast_to(index_row, (LANES, index_row.shape[1])))


def onehot_rows(index_cols, count):
    lane = lax.broadcasted_iota(jnp.int32, index_cols.shape, 1)
    blocks = [
        jnp.where(index_cols == lane + start, 1.0, 0.0).astype(BF16)
        for start in range(0, count, LANES)
    ]
    return jnp.concatenate(blocks, axis=1)


def pick(index_row, table):
    width = table.shape[1]
    high, low = split(table)
    both = dot(
        onehot_rows(down_lanes(index_row), table.shape[0]), jnp.concatenate([high, low], axis=1)
    )
    return both[:, :width] + both[:, width:]


def edge_terms(feats, weight):
    return lax.dot_general(
        feats,
        weight,
        (((0,), (0,)), ((), ())),
        precision=lax.Precision.HIGHEST,
        preferred_element_type=F32,
    )


def divide(value, count):
    if count & (count - 1) == 0:
        return value >> (count.bit_length() - 1), value & (count - 1)
    return value // count, value % count


VMEM = pl.BlockSpec(memory_space=pltpu.VMEM)


def call(body, outs, flops, args, scratch=()):
    return pl.pallas_call(
        body,
        out_shape=outs,
        in_specs=[VMEM] * len(args),
        out_specs=jax.tree.map(lambda _: VMEM, outs),
        scratch_shapes=scratch,
        compiler_params=pltpu.CompilerParams(vmem_limit_bytes=KERNEL_VMEM),
        cost_estimate=pl.CostEstimate(flops=flops, bytes_accessed=1 << 20, transcendentals=0),
    )(*args)


def shape(*dims, dtype=F32):
    return jax.ShapeDtypeStruct(dims, dtype)


def shift(value, axis, step):
    count = lax.axis_size(axis)
    return lax.ppermute(value, axis, [(i, (i + step) % count) for i in range(count)])


def swap_lat(value, first):
    count = lax.axis_size("lat")
    pairs = [(i, i + 1) for i in range(first, count - 1, 2)]
    return lax.ppermute(value, "lat", pairs + [(high, low) for low, high in pairs])


def by_role(value, lon_parity, lon_step, lat_first):
    lat_count, lon_count = lax.axis_size("lat"), lax.axis_size("lon")
    hid_count = lax.axis_size("hid")
    pairs = []
    for lat in range(lat_count):
        for lon in range(lon_count):
            for hid in range(hid_count):
                to_lat, to_lon = lat, lon
                if hid % 2 == lon_parity:
                    if lon_step is None:
                        continue
                    to_lon = (lon + lon_step) % lon_count
                else:
                    to_lat = lat_first + ((lat - lat_first) ^ 1)
                    if lat < lat_first or to_lat >= lat_count:
                        continue
                pairs.append(
                    (
                        (lat * lon_count + lon) * hid_count + hid,
                        (to_lat * lon_count + to_lon) * hid_count + hid,
                    )
                )
    return lax.ppermute(value, ("lat", "lon", "hid"), pairs)


def gather_hid(value):
    count = lax.axis_size("hid")
    pieces = [value]
    for step in range(1, count):
        source, hop = (pieces[step - 1], 1) if step % 2 else (value, step)
        pieces.append(lax.ppermute(source, "hid", [(i, i ^ hop) for i in range(count)]))
    return pieces


def layer_norm(message, gain, shift):
    centred = message - jnp.mean(message, axis=1, keepdims=True)
    spread = jnp.mean(centred * centred, axis=1, keepdims=True)
    return centred * lax.rsqrt(spread + epsilon) * gain + shift


def normed_chunks(hidden_refs, weight_ref, bias, gain, shift_row, store):
    edges = hidden_refs[0].shape[0]
    step = min(EDGE_CHUNK, edges)
    for start in range(0, edges, step):
        left = jnp.concatenate([ref[start : start + step, :] for ref in hidden_refs], axis=1)
        left_high, left_low = split(left)
        left = jnp.concatenate([left_high, left_high, left_low], axis=1)
        message = dot(left, weight_ref[...]) + bias
        store(start, step, layer_norm(message, gain, shift_row))


def aggregate(receiver_row, nodes, normed):
    node = lax.broadcasted_iota(jnp.int32, (nodes, receiver_row.shape[1]), 0)
    onehot = jnp.where(node == receiver_row, 1.0, 0.0).astype(BF16)
    width = normed.shape[1] // 2
    both = dot(onehot, normed)
    return both[:, :width] + both[:, width:]


def per_device(
    grid_latent,
    mesh_latent,
    grid_edge_feats,
    grid_senders,
    grid_receivers,
    mesh_edge_feats,
    mesh_senders,
    mesh_receivers,
    edge_weight,
    sender_weight,
    receiver_weight,
    first_bias,
    out_weight,
    out_bias,
    norm_gain,
    norm_shift,
):
    lon_count = lax.axis_size("lon")
    hid_count = lax.axis_size("hid")
    rows, cols, width = grid_latent.shape
    nodes = mesh_latent.shape[2]
    units = sender_weight.shape[2]
    grid_edges = grid_senders.shape[2]
    mesh_edges = mesh_senders.shape[2]
    mesh_own = mesh_latent.reshape(nodes, width)
    cells = grid_latent.reshape(rows * cols, width)
    grid_ids = grid_senders.reshape(1, grid_edges)
    grid_to = grid_receivers.reshape(1, grid_edges)
    mesh_ids = mesh_senders.reshape(1, mesh_edges)
    mesh_to = mesh_receivers.reshape(1, mesh_edges)
    two_lon = lon_count == 2
    id_rows = mesh_edges // LANES
    side_size = rows * 2 * RIM
    side_rows = side_size + id_rows + -(side_size + id_rows) % 8
    lat_size = RIM * cols + RIM * 2 * RIM
    lat_rows = lat_size + id_rows + -(lat_size + id_rows) % 16

    def local(receivers):
        patch = lax.axis_index("lat") * lon_count + lax.axis_index("lon")
        return receivers - patch * nodes

    def cell_places(ids):
        lat_index = lax.axis_index("lat")
        total_lon = cols * lon_count
        row, col = divide(ids, total_lon)
        row = row - lat_index * rows
        col = divide(col - lax.axis_index("lon") * cols + RIM, total_lon)[1] - RIM
        in_rows = (row >= 0) & (row < rows)
        in_cols = (col >= 0) & (col < cols)
        own = jnp.where(in_rows & in_cols, row * cols + col, -1)
        slot = jnp.where(col < 0, col + 2 * RIM, col - cols)
        rim_row = jnp.where(row < 0, row + RIM, row - rows)
        rim = jnp.where(in_cols, rim_row * cols + col, RIM * cols + rim_row * 2 * RIM + slot)
        odd = lat_index % 2
        rim = rim + side_size + jnp.where(row < 0, 1 - odd, odd) * lat_rows
        beyond = jnp.where(in_rows, jnp.where(in_cols, -1, row * 2 * RIM + slot), rim)
        return own, beyond

    def lat_partners():
        lat_index = lax.axis_index("lat")
        turn = 1 - 2 * (lat_index % 2)
        return lat_index + turn, lat_index - turn

    def sender_nodes(ids):
        source, node = divide(ids, nodes)
        source_lat, source_lon = divide(source, lon_count)
        offset = divide(source_lon - lax.axis_index("lon") + lon_count, lon_count)[1]
        tag = source_lat * lon_count + offset
        own = lax.axis_index("lat") * lon_count
        odd = lax.axis_index("hid") % 2 == 1
        first, second = lat_partners()
        first = jnp.where(odd, first * lon_count, own + (1 if two_lon else lon_count - 1))
        second = jnp.where(odd, second * lon_count, -1 if two_lon else own + 1)
        return [jnp.where(tag == place, node, -1) for place in (own, first, second)]

    def choose_ids(lat_ref, lat_start, lon_ref):
        odd = lax.axis_index("hid") % 2 == 1
        return jnp.where(odd, ids_in(lon_ref, side_size), ids_in(lat_ref, lat_start))

    def ids_in(ref, start):
        rows_of = [ref[start + row : start + row + 1, :] for row in range(id_rows)]
        return jnp.concatenate(rows_of, axis=1).astype(jnp.int32)

    def put_ids(ref, start, id_ref):
        ids = id_ref[...].astype(F32)
        for row in range(id_rows):
            ref[start + row : start + row + 1, :] = ids[:, row * LANES : (row + 1) * LANES]
        end = start + id_rows
        if end < ref.shape[0]:
            ref[end:, :] = jnp.zeros((ref.shape[0] - end, units), F32)

    def side_table(low_ref, high_ref):
        if two_lon:
            return low_ref[:side_size, :]
        slot = lax.broadcasted_iota(jnp.int32, (side_size, units), 0) % (2 * RIM)
        return jnp.where(slot < RIM, high_ref[:side_size, :], low_ref[:side_size, :])

    out_pieces = gather_hid(out_weight)

    chunk = rows * cols // 4

    def terms_body(
        cell_ref, weight_ref, id_ref, term_ref, side_ref, cell_vmem, weight_vmem, id_vmem, sems
    ):
        loads = [
            pltpu.make_async_copy(weight_ref.at[0], weight_vmem, sems.at[0]),
            pltpu.make_async_copy(id_ref, id_vmem, sems.at[1]),
        ]
        for step in range(4):
            part = pl.ds(step * chunk, chunk)
            loads.append(
                pltpu.make_async_copy(cell_ref.at[part], cell_vmem.at[part], sems.at[step + 2])
            )
        for load in loads:
            load.start()
        loads[0].wait()
        for step in range(4):
            loads[step + 2].wait()
            start = step * chunk
            term_ref[start : start + chunk, :] = dot_split(
                cell_vmem[start : start + chunk, :], weight_vmem[...]
            )
        loads[1].wait()
        put_ids(side_ref, side_size, id_vmem)
        for row in range(rows):
            start = row * 2 * RIM
            side_ref[start : start + RIM, :] = term_ref[row * cols : row * cols + RIM, :]
            side_ref[start + RIM : start + 2 * RIM, :] = term_ref[
                (row + 1) * cols - RIM : (row + 1) * cols, :
            ]

    hbm = pl.BlockSpec(memory_space=pltpu.HBM)
    terms, sides = pl.pallas_call(
        terms_body,
        out_shape=(shape(rows * cols, units), shape(side_rows, units)),
        in_specs=[hbm, hbm, hbm],
        out_specs=(VMEM, VMEM),
        scratch_shapes=[
            pltpu.VMEM((rows * cols, width), F32),
            pltpu.VMEM((width, units), F32),
            pltpu.VMEM((1, mesh_edges), jnp.int32),
            pltpu.SemaphoreType.DMA((6,)),
        ],
        name="grid_terms",
        compiler_params=pltpu.CompilerParams(vmem_limit_bytes=KERNEL_VMEM),
        cost_estimate=pl.CostEstimate(
            flops=6 * rows * cols * width * units, bytes_accessed=1 << 21, transcendentals=0
        ),
    )(
        pltpu.with_memory_space_constraint(cells, pltpu.HBM),
        pltpu.with_memory_space_constraint(sender_weight, pltpu.HBM),
        pltpu.with_memory_space_constraint(mesh_ids, pltpu.HBM),
    )
    side_low = shift(sides, "lon", 1)
    side_high = side_low if two_lon else shift(sides, "lon", -1)

    def grid_own_body(term_ref, feat_ref, edge_ref, bias_ref, send_ref, out_ref):
        out_ref[...] = (
            pick(cell_places(send_ref[...])[0], term_ref[...])
            + edge_terms(feat_ref[...], edge_ref[0])
            + bias_ref[0:1, :]
        )

    grid_pre = call(
        grid_own_body,
        shape(grid_edges, units),
        8 * grid_edges * rows * cols * units,
        (terms, grid_edge_feats.reshape(-1, grid_edges), edge_weight, first_bias, grid_ids),
    )

    def grid_received_body(pre_ref, mesh_ref, weight_ref, recv_ref, out_ref):
        received = dot_split(mesh_ref[...], weight_ref[0])
        out_ref[...] = pre_ref[...] + pick(local(recv_ref[...]), received)

    grid_pre = call(
        grid_received_body,
        shape(grid_edges, units),
        8 * grid_edges * rows * cols * units,
        (grid_pre, mesh_own, receiver_weight, grid_to),
    )

    def rim_body(term_ref, low_ref, high_ref, id_ref, a_ref, b_ref):
        odd = lax.axis_index("lat") % 2
        table = side_table(low_ref, high_ref)
        for ref, up in ((a_ref, 1 - odd), (b_ref, odd)):
            start = up * (rows - RIM)
            ref[: RIM * cols, :] = term_ref[pl.ds(pl.multiple_of(start * cols, 8), RIM * cols), :]
            ref[RIM * cols : lat_size, :] = jnp.where(
                up == 1, table[(rows - RIM) * 2 * RIM :, :], table[: RIM * 2 * RIM, :]
            )
            put_ids(ref, lat_size, id_ref)

    rim_block = shape(lat_rows, units)
    rim_a, rim_b = call(
        rim_body, (rim_block, rim_block), 1 << 20, (terms, side_low, side_high, mesh_ids)
    )
    rim_a = swap_lat(rim_a, 0)
    rim_b = swap_lat(rim_b, 1)

    halves = [shape(grid_edges // 2, units)] * 2

    def grid_hidden_body(pre_ref, low_ref, high_ref, a_ref, b_ref, send_ref, *hidden_refs):
        pad = -(side_size + 2 * lat_rows) % LANES
        table = jnp.concatenate(
            [side_table(low_ref, high_ref), a_ref[...], b_ref[...], jnp.zeros((pad, units), F32)],
            axis=0,
        )
        total = pre_ref[...] + pick(cell_places(send_ref[...])[1], table)
        total = total / (1.0 + jnp.exp(-total))
        for half, ref in enumerate(hidden_refs):
            ref[...] = total[half * ref.shape[0] : (half + 1) * ref.shape[0], :]

    grid_hidden = call(
        grid_hidden_body,
        tuple(halves),
        4 * grid_edges * rows * cols * units,
        (grid_pre, side_low, side_high, rim_a, rim_b, grid_ids),
    )
    grid_pieces = [gather_hid(part) for part in grid_hidden]

    def weight_body(*refs):
        for section in range(2):
            whole = jnp.concatenate([ref[section] for ref in refs[:hid_count]], axis=0)
            high, low = split(whole)
            out_ref = refs[hid_count + section]
            out_ref[:width, :] = high
            out_ref[width : 2 * width, :] = low
            out_ref[2 * width :, :] = high

    weight_block = shape(3 * width, width, dtype=BF16)
    grid_weight, mesh_weight = call(weight_body, (weight_block, weight_block), 1 << 28, out_pieces)

    def grid_message_body(*refs):
        hidden_refs = refs[:hid_count]
        weight_ref, bias_ref, gain_ref, shift_ref, normed_ref = refs[hid_count:]

        def store(start, step, normed):
            high, low = split(normed)
            normed_ref[start : start + step, :width] = high
            normed_ref[start : start + step, width:] = low

        normed_chunks(
            hidden_refs, weight_ref, bias_ref[0:1, :], gain_ref[0:1, :], shift_ref[0:1, :], store
        )

    normed_parts = [
        call(
            grid_message_body,
            shape(grid_edges // 2, 2 * width, dtype=BF16),
            4 * grid_edges * width * width,
            (*pieces, grid_weight, out_bias, norm_gain, norm_shift),
        )
        for pieces in grid_pieces
    ]

    def grid_sum_body(first_ref, second_ref, recv_ref, mesh_ref, send_ref, mid_ref, term_ref):
        normed = jnp.concatenate([first_ref[...], second_ref[...]], axis=0)
        middle = mesh_ref[...] + aggregate(local(recv_ref[...]), nodes, normed)
        mid_ref[...] = middle
        term_ref[...] = dot_split(middle, send_ref[1])

    mesh_mid, mesh_terms = call(
        grid_sum_body,
        (shape(nodes, width), shape(nodes, units)),
        4 * grid_edges * width * width,
        (*normed_parts, grid_to, mesh_own, sender_weight),
    )

    back = None if two_lon else -1
    table_a = by_role(mesh_terms, 0, 1, 0)
    table_b = by_role(mesh_terms, 0, back, 1)

    def mesh_first_body(
        term_ref, mid_ref, weight_ref, feat_ref, edge_ref, bias_ref, recv_ref, id_ref,
        rim_a_ref, rim_b_ref, low_ref, high_ref, pre_ref, a_ref, b_ref,
    ):
        table = term_ref[...]
        a_ref[...] = pick(sender_nodes(choose_ids(rim_a_ref, lat_size, high_ref))[0], table)
        b_ref[...] = pick(sender_nodes(choose_ids(rim_b_ref, lat_size, low_ref))[0], table)
        received = dot_split(mid_ref[...], weight_ref[1])
        pre_ref[...] = (
            pick(sender_nodes(id_ref[...])[0], table)
            + pick(local(recv_ref[...]), received)
            + edge_terms(feat_ref[...], edge_ref[1])
            + bias_ref[1:2, :]
        )

    edge_block = shape(mesh_edges, units)
    mesh_pre, send_a, send_b = call(
        mesh_first_body,
        (edge_block, edge_block, edge_block),
        16 * mesh_edges * nodes * units,
        (
            mesh_terms, mesh_mid, receiver_weight, mesh_edge_feats.reshape(-1, mesh_edges), edge_weight,
            first_bias, mesh_to, mesh_ids, rim_a, rim_b, side_low, side_high,
        ),
    )

    def add_others(first_ref, ids, table_refs):
        total = first_ref[...]
        for index_row, table_ref in zip(sender_nodes(ids)[1:], table_refs):
            total = total + pick(index_row, table_ref[...])
        return total

    def mesh_sent_body(
        table_a_ref, table_b_ref, first_a, first_b, rim_a_ref, rim_b_ref, low_ref, high_ref, a_ref, b_ref
    ):
        tables = (table_a_ref, table_b_ref)
        a_ref[...] = add_others(first_a, choose_ids(rim_a_ref, lat_size, high_ref), tables)
        b_ref[...] = add_others(first_b, choose_ids(rim_b_ref, lat_size, low_ref), tables)

    send_a, send_b = call(
        mesh_sent_body,
        (edge_block, edge_block),
        16 * mesh_edges * nodes * units,
        (table_a, table_b, send_a, send_b, rim_a, rim_b, side_low, side_high),
    )
    got_a = by_role(send_a, 1, 1, 0)
    got_b = by_role(send_b, 1, back, 1)

    def mesh_own_body(table_a_ref, table_b_ref, first_ref, id_ref, out_ref):
        out_ref[...] = add_others(first_ref, id_ref[...], (table_a_ref, table_b_ref))

    mesh_pre = call(
        mesh_own_body,
        edge_block,
        8 * mesh_edges * nodes * units,
        (table_a, table_b, mesh_pre, mesh_ids),
    )
    total = mesh_pre + got_a + got_b
    mesh_pieces = gather_hid(total / (1.0 + jnp.exp(-total)))
    share = width // hid_count

    def mesh_message_body(*refs):
        hidden_refs = refs[:hid_count]
        weight_ref, bias_ref, gain_ref, shift_ref, recv_ref, mid_ref, out_ref, normed_ref = refs[hid_count:]
        place = lax.axis_index("hid")

        def own_part(value):
            part = value[:, :share]
            for step in range(1, hid_count):
                part = jnp.where(place == step, value[:, step * share : (step + 1) * share], part)
            return part

        def store(start, step, normed):
            high, low = split(own_part(normed))
            normed_ref[start : start + step, :share] = high
            normed_ref[start : start + step, share:] = low

        normed_chunks(
            hidden_refs, weight_ref, bias_ref[1:2, :], gain_ref[1:2, :], shift_ref[1:2, :], store
        )
        out_ref[...] = own_part(mid_ref[...]) + aggregate(local(recv_ref[...]), nodes, normed_ref[...])

    mesh_out = call(
        mesh_message_body,
        shape(nodes, share),
        8 * mesh_edges * width * width,
        (*mesh_pieces, mesh_weight, out_bias, norm_gain, norm_shift, mesh_to, mesh_mid),
        (pltpu.VMEM((mesh_edges, 2 * share), BF16),),
    )
    return mesh_out.reshape(1, 1, nodes, share)


def solution(mesh):
    return jax.shard_map(
        per_device,
        mesh=mesh,
        in_specs=(
            P("lat", "lon", None),
            P("lat", "lon", None, None),
            P("lat", "lon", None, None),
            P("lat", "lon", None),
            P("lat", "lon", None),
            P("lat", "lon", None, None),
            P("lat", "lon", None),
            P("lat", "lon", None),
            P(None, None, "hid"),
            P(None, None, "hid"),
            P(None, None, "hid"),
            P(None, "hid"),
            P(None, "hid", None),
            P(),
            P(),
            P(),
        ),
        out_specs=P("lat", "lon", None, "hid"),
        check_vma=False,
    )
```

```python
import jax
import jax.numpy as jnp
from jax import lax
from jax.experimental import pallas as pl
from jax.experimental.pallas import tpu as pltpu
from jax.sharding import PartitionSpec as P

RIM = 2
LANES = 128
EDGE_CHUNK = 256
KERNEL_VMEM = 24 << 20
epsilon = 1e-05
F32 = jnp.float32
BF16 = jnp.bfloat16


def split(value):
    high = value.astype(BF16)
    low = (value - high.astype(F32)).astype(BF16)
    return high, low


def dot(left, right):
    return jnp.dot(left, right, preferred_element_type=F32)


def dot_split(left, right):
    left_high, left_low = split(left)
    right_high, right_low = split(right)
    return dot(
        jnp.concatenate([left_high, left_high, left_low], axis=1),
        jnp.concatenate([right_high, right_low, right_high], axis=0),
    )


def down_lanes(index_row):
    return jnp.transpose(jnp.broadcast_to(index_row, (LANES, index_row.shape[1])))


def onehot_rows(index_cols, count):
    lane = lax.broadcasted_iota(jnp.int32, index_cols.shape, 1)
    blocks = [
        jnp.where(index_cols == lane + start, 1.0, 0.0).astype(BF16)
        for start in range(0, count, LANES)
    ]
    return jnp.concatenate(blocks, axis=1)


def pick(index_row, table):
    width = table.shape[1]
    high, low = split(table)
    both = dot(
        onehot_rows(down_lanes(index_row), table.shape[0]), jnp.concatenate([high, low], axis=1)
    )
    return both[:, :width] + both[:, width:]


def edge_terms(feats, weight):
    return lax.dot_general(
        feats,
        weight,
        (((0,), (0,)), ((), ())),
        precision=lax.Precision.HIGHEST,
        preferred_element_type=F32,
    )


def divide(value, count):
    if count & (count - 1) == 0:
        return value >> (count.bit_length() - 1), value & (count - 1)
    return value // count, value % count


VMEM = pl.BlockSpec(memory_space=pltpu.VMEM)


def call(body, outs, flops, args, scratch=()):
    return pl.pallas_call(
        body,
        out_shape=outs,
        in_specs=[VMEM] * len(args),
        out_specs=jax.tree.map(lambda _: VMEM, outs),
        scratch_shapes=scratch,
        compiler_params=pltpu.CompilerParams(vmem_limit_bytes=KERNEL_VMEM),
        cost_estimate=pl.CostEstimate(flops=flops, bytes_accessed=1 << 20, transcendentals=0),
    )(*args)


def shape(*dims, dtype=F32):
    return jax.ShapeDtypeStruct(dims, dtype)


def shift(value, axis, step):
    count = lax.axis_size(axis)
    return lax.ppermute(value, axis, [(i, (i + step) % count) for i in range(count)])


def exchange(value, target_of):
    sizes = [lax.axis_size(axis) for axis in ("lat", "lon", "hid")]
    places = [
        (lat, lon, hid) for lat in range(sizes[0]) for lon in range(sizes[1]) for hid in range(sizes[2])
    ]
    targets = {place: target_of(*place) for place in places}
    idle = {place for place, target in targets.items() if target is None}
    for hop in (1, 2):
        for lat, lon, hid in sorted(idle):
            other = (lat, lon, hid ^ hop)
            if (lat, lon, hid) in idle and other in idle:
                targets[lat, lon, hid], targets[other] = other, (lat, lon, hid)
                idle -= {(lat, lon, hid), other}
    numbers = {place: number for number, place in enumerate(places)}
    pairs = [(numbers[source], numbers[target]) for source, target in targets.items() if target]
    return lax.ppermute(value, ("lat", "lon", "hid"), pairs)


def lat_partner(lat, first):
    other = first + ((lat - first) ^ 1)
    return other if lat >= first and other < lax.axis_size("lat") else None


def swap_lat(value, first):
    def target(lat, lon, hid):
        other = lat_partner(lat, first)
        return None if other is None else (other, lon, hid)

    return exchange(value, target)


def by_role(value, lon_parity, lon_step, lat_first):
    lon_count = lax.axis_size("lon")

    def target(lat, lon, hid):
        if hid % 2 == lon_parity:
            return None if lon_step is None else (lat, (lon + lon_step) % lon_count, hid)
        other = lat_partner(lat, lat_first)
        return None if other is None else (other, lon, hid)

    return exchange(value, target)


def gather_hid(value):
    count = lax.axis_size("hid")
    pieces = [value]
    for step in range(1, count):
        source, hop = (pieces[step - 1], 1) if step % 2 else (value, step)
        pieces.append(lax.ppermute(source, "hid", [(i, i ^ hop) for i in range(count)]))
    return pieces


def layer_norm(message, gain, shift):
    centred = message - jnp.mean(message, axis=1, keepdims=True)
    spread = jnp.mean(centred * centred, axis=1, keepdims=True)
    return centred * lax.rsqrt(spread + epsilon) * gain + shift


def normed_chunks(hidden_refs, weight_ref, bias, gain, shift_row, store):
    edges = hidden_refs[0].shape[0]
    step = min(EDGE_CHUNK, edges)
    for start in range(0, edges, step):
        left = jnp.concatenate([ref[start : start + step, :] for ref in hidden_refs], axis=1)
        left_high, left_low = split(left)
        left = jnp.concatenate([left_high, left_high, left_low], axis=1)
        message = dot(left, weight_ref[...]) + bias
        store(start, step, layer_norm(message, gain, shift_row))


def aggregate(receiver_row, nodes, normed):
    node = lax.broadcasted_iota(jnp.int32, (nodes, receiver_row.shape[1]), 0)
    onehot = jnp.where(node == receiver_row, 1.0, 0.0).astype(BF16)
    width = normed.shape[1] // 2
    both = dot(onehot, normed)
    return both[:, :width] + both[:, width:]


def per_device(
    grid_latent,
    mesh_latent,
    grid_edge_feats,
    grid_senders,
    grid_receivers,
    mesh_edge_feats,
    mesh_senders,
    mesh_receivers,
    edge_weight,
    sender_weight,
    receiver_weight,
    first_bias,
    out_weight,
    out_bias,
    norm_gain,
    norm_shift,
):
    lon_count = lax.axis_size("lon")
    hid_count = lax.axis_size("hid")
    rows, cols, width = grid_latent.shape
    nodes = mesh_latent.shape[2]
    units = sender_weight.shape[2]
    grid_edges = grid_senders.shape[2]
    mesh_edges = mesh_senders.shape[2]
    mesh_own = mesh_latent.reshape(nodes, width)
    cells = grid_latent.reshape(rows * cols, width)
    grid_ids = grid_senders.reshape(1, grid_edges)
    grid_to = grid_receivers.reshape(1, grid_edges)
    mesh_ids = mesh_senders.reshape(1, mesh_edges)
    mesh_to = mesh_receivers.reshape(1, mesh_edges)
    two_lon = lon_count == 2
    id_rows = mesh_edges // LANES
    side_size = rows * 2 * RIM
    side_rows = side_size + id_rows + -(side_size + id_rows) % 8
    lat_size = RIM * cols + RIM * 2 * RIM
    lat_rows = lat_size + id_rows + -(lat_size + id_rows) % 16

    def local(receivers):
        patch = lax.axis_index("lat") * lon_count + lax.axis_index("lon")
        return receivers - patch * nodes

    def cell_places(ids):
        lat_index = lax.axis_index("lat")
        total_lon = cols * lon_count
        row, col = divide(ids, total_lon)
        row = row - lat_index * rows
        col = divide(col - lax.axis_index("lon") * cols + RIM, total_lon)[1] - RIM
        in_rows = (row >= 0) & (row < rows)
        in_cols = (col >= 0) & (col < cols)
        own = jnp.where(in_rows & in_cols, row * cols + col, -1)
        slot = jnp.where(col < 0, col + 2 * RIM, col - cols)
        rim_row = jnp.where(row < 0, row + RIM, row - rows)
        rim = jnp.where(in_cols, rim_row * cols + col, RIM * cols + rim_row * 2 * RIM + slot)
        odd = lat_index % 2
        rim = rim + side_size + jnp.where(row < 0, 1 - odd, odd) * lat_rows
        beyond = jnp.where(in_rows, jnp.where(in_cols, -1, row * 2 * RIM + slot), rim)
        return own, beyond

    def lat_partners():
        lat_index = lax.axis_index("lat")
        turn = 1 - 2 * (lat_index % 2)
        return lat_index + turn, lat_index - turn

    def sender_nodes(ids):
        source, node = divide(ids, nodes)
        source_lat, source_lon = divide(source, lon_count)
        offset = divide(source_lon - lax.axis_index("lon") + lon_count, lon_count)[1]
        tag = source_lat * lon_count + offset
        own = lax.axis_index("lat") * lon_count
        odd = lax.axis_index("hid") % 2 == 1
        first, second = lat_partners()
        first = jnp.where(odd, first * lon_count, own + (1 if two_lon else lon_count - 1))
        second = jnp.where(odd, second * lon_count, -1 if two_lon else own + 1)
        return [jnp.where(tag == place, node, -1) for place in (own, first, second)]

    def choose_ids(way, lat_ref, lon_ref):
        odd = lax.axis_index("hid") % 2 == 1
        partner = lat_partners()[way]
        along_lat = jnp.where((partner >= 0) & (partner < lax.axis_size("lat")), 1, 0)
        valid = jnp.where(odd, 0 if two_lon and way == 1 else 1, along_lat)
        ids = jnp.where(odd, ids_in(lon_ref, side_size), ids_in(lat_ref, lat_size))
        return jnp.where(valid == 1, ids, -4 * nodes * lon_count)

    def ids_in(ref, start):
        rows_of = [ref[start + row : start + row + 1, :] for row in range(id_rows)]
        return jnp.concatenate(rows_of, axis=1).astype(jnp.int32)

    def put_ids(ref, start, id_ref):
        ids = id_ref[...].astype(F32)
        for row in range(id_rows):
            ref[start + row : start + row + 1, :] = ids[:, row * LANES : (row + 1) * LANES]
        end = start + id_rows
        if end < ref.shape[0]:
            ref[end:, :] = jnp.zeros((ref.shape[0] - end, units), F32)

    def side_table(low_ref, high_ref):
        if two_lon:
            return low_ref[:side_size, :]
        slot = lax.broadcasted_iota(jnp.int32, (side_size, units), 0) % (2 * RIM)
        return jnp.where(slot < RIM, high_ref[:side_size, :], low_ref[:side_size, :])

    out_pieces = gather_hid(out_weight)

    chunk = rows * cols // 4

    def terms_body(
        cell_ref, weight_ref, id_ref, term_ref, side_ref, cell_vmem, weight_vmem, id_vmem, sems
    ):
        loads = [
            pltpu.make_async_copy(weight_ref.at[0], weight_vmem, sems.at[0]),
            pltpu.make_async_copy(id_ref, id_vmem, sems.at[1]),
        ]
        for step in range(4):
            part = pl.ds(step * chunk, chunk)
            loads.append(
                pltpu.make_async_copy(cell_ref.at[part], cell_vmem.at[part], sems.at[step + 2])
            )
        for load in loads:
            load.start()
        loads[0].wait()
        for step in range(4):
            loads[step + 2].wait()
            start = step * chunk
            term_ref[start : start + chunk, :] = dot_split(
                cell_vmem[start : start + chunk, :], weight_vmem[...]
            )
        loads[1].wait()
        put_ids(side_ref, side_size, id_vmem)
        for row in range(rows):
            start = row * 2 * RIM
            side_ref[start : start + RIM, :] = term_ref[row * cols : row * cols + RIM, :]
            side_ref[start + RIM : start + 2 * RIM, :] = term_ref[
                (row + 1) * cols - RIM : (row + 1) * cols, :
            ]

    hbm = pl.BlockSpec(memory_space=pltpu.HBM)
    terms, sides = pl.pallas_call(
        terms_body,
        out_shape=(shape(rows * cols, units), shape(side_rows, units)),
        in_specs=[hbm, hbm, hbm],
        out_specs=(VMEM, VMEM),
        scratch_shapes=[
            pltpu.VMEM((rows * cols, width), F32),
            pltpu.VMEM((width, units), F32),
            pltpu.VMEM((1, mesh_edges), jnp.int32),
            pltpu.SemaphoreType.DMA((6,)),
        ],
        name="grid_terms",
        compiler_params=pltpu.CompilerParams(vmem_limit_bytes=KERNEL_VMEM),
        cost_estimate=pl.CostEstimate(
            flops=6 * rows * cols * width * units, bytes_accessed=1 << 21, transcendentals=0
        ),
    )(
        pltpu.with_memory_space_constraint(cells, pltpu.HBM),
        pltpu.with_memory_space_constraint(sender_weight, pltpu.HBM),
        pltpu.with_memory_space_constraint(mesh_ids, pltpu.HBM),
    )
    side_low = shift(sides, "lon", 1)
    side_high = side_low if two_lon else shift(sides, "lon", -1)

    def grid_own_body(term_ref, feat_ref, edge_ref, bias_ref, send_ref, out_ref):
        out_ref[...] = (
            pick(cell_places(send_ref[...])[0], term_ref[...])
            + edge_terms(feat_ref[...], edge_ref[0])
            + bias_ref[0:1, :]
        )

    grid_pre = call(
        grid_own_body,
        shape(grid_edges, units),
        8 * grid_edges * rows * cols * units,
        (terms, grid_edge_feats.reshape(-1, grid_edges), edge_weight, first_bias, grid_ids),
    )

    def grid_received_body(pre_ref, mesh_ref, weight_ref, recv_ref, out_ref):
        received = dot_split(mesh_ref[...], weight_ref[0])
        out_ref[...] = pre_ref[...] + pick(local(recv_ref[...]), received)

    grid_pre = call(
        grid_received_body,
        shape(grid_edges, units),
        8 * grid_edges * rows * cols * units,
        (grid_pre, mesh_own, receiver_weight, grid_to),
    )

    def rim_body(term_ref, low_ref, high_ref, id_ref, a_ref, b_ref):
        odd = lax.axis_index("lat") % 2
        table = side_table(low_ref, high_ref)
        for ref, up in ((a_ref, 1 - odd), (b_ref, odd)):
            start = up * (rows - RIM)
            ref[: RIM * cols, :] = term_ref[pl.ds(pl.multiple_of(start * cols, 8), RIM * cols), :]
            ref[RIM * cols : lat_size, :] = jnp.where(
                up == 1, table[(rows - RIM) * 2 * RIM :, :], table[: RIM * 2 * RIM, :]
            )
            put_ids(ref, lat_size, id_ref)

    rim_block = shape(lat_rows, units)
    rim_a, rim_b = call(rim_body, (rim_block, rim_block), 1 << 20, (terms, side_low, side_high, mesh_ids))
    rim_a = swap_lat(rim_a, 0)
    rim_b = swap_lat(rim_b, 1)

    halves = [shape(grid_edges // 2, units)] * 2

    def grid_hidden_body(pre_ref, low_ref, high_ref, a_ref, b_ref, send_ref, *hidden_refs):
        pad = -(side_size + 2 * lat_rows) % LANES
        table = jnp.concatenate(
            [side_table(low_ref, high_ref), a_ref[...], b_ref[...], jnp.zeros((pad, units), F32)],
            axis=0,
        )
        total = pre_ref[...] + pick(cell_places(send_ref[...])[1], table)
        total = total / (1.0 + jnp.exp(-total))
        for half, ref in enumerate(hidden_refs):
            ref[...] = total[half * ref.shape[0] : (half + 1) * ref.shape[0], :]

    grid_hidden = call(
        grid_hidden_body,
        tuple(halves),
        4 * grid_edges * rows * cols * units,
        (grid_pre, side_low, side_high, rim_a, rim_b, grid_ids),
    )
    grid_pieces = [gather_hid(part) for part in grid_hidden]

    def weight_body(*refs):
        for section in range(2):
            whole = jnp.concatenate([ref[section] for ref in refs[:hid_count]], axis=0)
            high, low = split(whole)
            out_ref = refs[hid_count + section]
            out_ref[:width, :] = high
            out_ref[width : 2 * width, :] = low
            out_ref[2 * width :, :] = high

    weight_block = shape(3 * width, width, dtype=BF16)
    grid_weight, mesh_weight = call(weight_body, (weight_block, weight_block), 1 << 28, out_pieces)

    half_edges = grid_edges // 2

    def half_sum(half, refs, normed_ref):
        hidden_refs = refs[:hid_count]
        weight_ref, bias_ref, gain_ref, shift_ref, recv_ref = refs[hid_count : hid_count + 5]

        def store(start, step, normed):
            high, low = split(normed)
            normed_ref[start : start + step, :width] = high
            normed_ref[start : start + step, width:] = low

        normed_chunks(
            hidden_refs, weight_ref, bias_ref[0:1, :], gain_ref[0:1, :], shift_ref[0:1, :], store
        )
        receivers = recv_ref[:, half * half_edges : (half + 1) * half_edges]
        return aggregate(local(receivers), nodes, normed_ref[...])

    def grid_first_half_body(*refs):
        mesh_ref, sum_ref, normed_ref = refs[-3:]
        sum_ref[...] = mesh_ref[...] + half_sum(0, refs, normed_ref)

    def grid_second_half_body(*refs):
        first_ref, send_ref, mid_ref, term_ref, normed_ref = refs[-5:]
        middle = first_ref[...] + half_sum(1, refs, normed_ref)
        mid_ref[...] = middle
        term_ref[...] = dot_split(middle, send_ref[1])

    normed_scratch = (pltpu.VMEM((half_edges, 2 * width), BF16),)
    shared = (grid_weight, out_bias, norm_gain, norm_shift, grid_to)
    first_sum = call(
        grid_first_half_body,
        shape(nodes, width),
        5 * grid_edges * width * width,
        (*grid_pieces[0], *shared, mesh_own),
        normed_scratch,
    )
    mesh_mid, mesh_terms = call(
        grid_second_half_body,
        (shape(nodes, width), shape(nodes, units)),
        6 * grid_edges * width * width,
        (*grid_pieces[1], *shared, first_sum, sender_weight),
        normed_scratch,
    )

    back = None if two_lon else -1
    table_a = by_role(mesh_terms, 0, 1, 0)
    table_b = by_role(mesh_terms, 0, back, 1)

    def mesh_first_body(
        term_ref, mid_ref, weight_ref, feat_ref, edge_ref, bias_ref, recv_ref, id_ref,
        rim_a_ref, rim_b_ref, low_ref, high_ref, pre_ref, a_ref, b_ref,
    ):
        table = term_ref[...]
        a_ref[...] = pick(sender_nodes(choose_ids(0, rim_a_ref, high_ref))[0], table)
        b_ref[...] = pick(sender_nodes(choose_ids(1, rim_b_ref, low_ref))[0], table)
        received = dot_split(mid_ref[...], weight_ref[1])
        pre_ref[...] = (
            pick(sender_nodes(id_ref[...])[0], table)
            + pick(local(recv_ref[...]), received)
            + edge_terms(feat_ref[...], edge_ref[1])
            + bias_ref[1:2, :]
        )

    edge_block = shape(mesh_edges, units)
    mesh_pre, send_a, send_b = call(
        mesh_first_body,
        (edge_block, edge_block, edge_block),
        16 * mesh_edges * nodes * units,
        (
            mesh_terms, mesh_mid, receiver_weight, mesh_edge_feats.reshape(-1, mesh_edges), edge_weight,
            first_bias, mesh_to, mesh_ids, rim_a, rim_b, side_low, side_high,
        ),
    )

    def add_others(first_ref, ids, table_refs):
        total = first_ref[...]
        for index_row, table_ref in zip(sender_nodes(ids)[1:], table_refs):
            total = total + pick(index_row, table_ref[...])
        return total

    def mesh_sent_body(
        table_a_ref, table_b_ref, first_a, first_b, rim_a_ref, rim_b_ref, low_ref, high_ref, a_ref, b_ref
    ):
        tables = (table_a_ref, table_b_ref)
        a_ref[...] = add_others(first_a, choose_ids(0, rim_a_ref, high_ref), tables)
        b_ref[...] = add_others(first_b, choose_ids(1, rim_b_ref, low_ref), tables)

    send_a, send_b = call(
        mesh_sent_body,
        (edge_block, edge_block),
        16 * mesh_edges * nodes * units,
        (table_a, table_b, send_a, send_b, rim_a, rim_b, side_low, side_high),
    )
    got_a = by_role(send_a, 1, 1, 0)
    got_b = by_role(send_b, 1, back, 1)

    def mesh_own_body(table_a_ref, table_b_ref, first_ref, id_ref, out_ref):
        out_ref[...] = add_others(first_ref, id_ref[...], (table_a_ref, table_b_ref))

    mesh_pre = call(mesh_own_body, edge_block, 8 * mesh_edges * nodes * units, (table_a, table_b, mesh_pre, mesh_ids))
    total = mesh_pre + got_a + got_b
    mesh_pieces = gather_hid(total / (1.0 + jnp.exp(-total)))
    share = width // hid_count

    def mesh_message_body(*refs):
        hidden_refs = refs[:hid_count]
        weight_ref, bias_ref, gain_ref, shift_ref, recv_ref, mid_ref, out_ref, normed_ref = refs[hid_count:]
        place = lax.axis_index("hid")

        def own_part(value):
            part = value[:, :share]
            for step in range(1, hid_count):
                part = jnp.where(place == step, value[:, step * share : (step + 1) * share], part)
            return part

        def store(start, step, normed):
            high, low = split(own_part(normed))
            normed_ref[start : start + step, :share] = high
            normed_ref[start : start + step, share:] = low

        normed_chunks(
            hidden_refs, weight_ref, bias_ref[1:2, :], gain_ref[1:2, :], shift_ref[1:2, :], store
        )
        out_ref[...] = own_part(mid_ref[...]) + aggregate(local(recv_ref[...]), nodes, normed_ref[...])

    mesh_out = call(
        mesh_message_body,
        shape(nodes, share),
        8 * mesh_edges * width * width,
        (*mesh_pieces, mesh_weight, out_bias, norm_gain, norm_shift, mesh_to, mesh_mid),
        (pltpu.VMEM((mesh_edges, 2 * share), BF16),),
    )
    return mesh_out.reshape(1, 1, nodes, share)


def solution(mesh):
    return jax.shard_map(
        per_device,
        mesh=mesh,
        in_specs=(
            P("lat", "lon", None),
            P("lat", "lon", None, None),
            P("lat", "lon", None, None),
            P("lat", "lon", None),
            P("lat", "lon", None),
            P("lat", "lon", None, None),
            P("lat", "lon", None),
            P("lat", "lon", None),
            P(None, None, "hid"),
            P(None, None, "hid"),
            P(None, None, "hid"),
            P(None, "hid"),
            P(None, "hid", None),
            P(),
            P(),
            P(),
        ),
        out_specs=P("lat", "lon", None, "hid"),
        check_vma=False,
    )
```

```python
import jax
import jax.numpy as jnp
from jax import lax
from jax.experimental import pallas as pl
from jax.experimental.pallas import tpu as pltpu
from jax.sharding import PartitionSpec as P

RIM = 2
LANES = 128
EDGE_CHUNK = 256
KERNEL_VMEM = 24 << 20
epsilon = 1e-05
F32 = jnp.float32
BF16 = jnp.bfloat16


def split(value):
    high = value.astype(BF16)
    low = (value - high.astype(F32)).astype(BF16)
    return high, low


def dot(left, right):
    return jnp.dot(left, right, preferred_element_type=F32)


def dot_split(left, right):
    left_high, left_low = split(left)
    right_high, right_low = split(right)
    return dot(
        jnp.concatenate([left_high, left_high, left_low], axis=1),
        jnp.concatenate([right_high, right_low, right_high], axis=0),
    )


def down_lanes(index_row):
    return jnp.transpose(jnp.broadcast_to(index_row, (LANES, index_row.shape[1])))


def onehot_rows(index_cols, count):
    lane = lax.broadcasted_iota(jnp.int32, index_cols.shape, 1)
    blocks = [
        jnp.where(index_cols == lane + start, 1.0, 0.0).astype(BF16)
        for start in range(0, count, LANES)
    ]
    return jnp.concatenate(blocks, axis=1)


def pick_hot(onehot, table):
    width = table.shape[1]
    high, low = split(table)
    both = dot(onehot, jnp.concatenate([high, low], axis=1))
    return both[:, :width] + both[:, width:]


def pick(index_row, table):
    return pick_hot(onehot_rows(down_lanes(index_row), table.shape[0]), table)


def edge_terms(feats, weight):
    return lax.dot_general(
        feats,
        weight,
        (((0,), (0,)), ((), ())),
        precision=lax.Precision.HIGHEST,
        preferred_element_type=F32,
    )


def divide(value, count):
    if count & (count - 1) == 0:
        return value >> (count.bit_length() - 1), value & (count - 1)
    return value // count, value % count


VMEM = pl.BlockSpec(memory_space=pltpu.VMEM)


def call(body, outs, flops, args, scratch=()):
    return pl.pallas_call(
        body,
        out_shape=outs,
        in_specs=[VMEM] * len(args),
        out_specs=jax.tree.map(lambda _: VMEM, outs),
        scratch_shapes=scratch,
        compiler_params=pltpu.CompilerParams(vmem_limit_bytes=KERNEL_VMEM),
        cost_estimate=pl.CostEstimate(flops=flops, bytes_accessed=1 << 20, transcendentals=0),
    )(*args)


def shape(*dims, dtype=F32):
    return jax.ShapeDtypeStruct(dims, dtype)


def shift(value, axis, step):
    count = lax.axis_size(axis)
    return lax.ppermute(value, axis, [(i, (i + step) % count) for i in range(count)])


def exchange(value, target_of):
    sizes = [lax.axis_size(axis) for axis in ("lat", "lon", "hid")]
    places = [
        (lat, lon, hid) for lat in range(sizes[0]) for lon in range(sizes[1]) for hid in range(sizes[2])
    ]
    targets = {place: target_of(*place) for place in places}
    idle = {place for place, target in targets.items() if target is None}
    for hop in (1, 2):
        for lat, lon, hid in sorted(idle):
            other = (lat, lon, hid ^ hop)
            if (lat, lon, hid) in idle and other in idle:
                targets[lat, lon, hid], targets[other] = other, (lat, lon, hid)
                idle -= {(lat, lon, hid), other}
    numbers = {place: number for number, place in enumerate(places)}
    pairs = [(numbers[source], numbers[target]) for source, target in targets.items() if target]
    return lax.ppermute(value, ("lat", "lon", "hid"), pairs)


def lat_partner(lat, first):
    other = first + ((lat - first) ^ 1)
    return other if lat >= first and other < lax.axis_size("lat") else None


def swap_lat(value, first):
    def target(lat, lon, hid):
        other = lat_partner(lat, first)
        return None if other is None else (other, lon, hid)

    return exchange(value, target)


def by_role(value, lon_parity, lon_step, lat_first):
    lon_count = lax.axis_size("lon")

    def target(lat, lon, hid):
        if hid % 2 == lon_parity:
            return None if lon_step is None else (lat, (lon + lon_step) % lon_count, hid)
        other = lat_partner(lat, lat_first)
        return None if other is None else (other, lon, hid)

    return exchange(value, target)


def gather_hid(value):
    count = lax.axis_size("hid")
    pieces = [value]
    for step in range(1, count):
        source, hop = (pieces[step - 1], 1) if step % 2 else (value, step)
        pieces.append(lax.ppermute(source, "hid", [(i, i ^ hop) for i in range(count)]))
    return pieces


def layer_norm(message, gain, shift):
    centred = message - jnp.mean(message, axis=1, keepdims=True)
    spread = jnp.mean(centred * centred, axis=1, keepdims=True)
    return centred * lax.rsqrt(spread + epsilon) * gain + shift


def normed_chunks(hidden_refs, weight_ref, bias, gain, shift_row, store):
    edges = hidden_refs[0].shape[0]
    step = min(EDGE_CHUNK, edges)
    for start in range(0, edges, step):
        left = jnp.concatenate([ref[start : start + step, :] for ref in hidden_refs], axis=1)
        left_high, left_low = split(left)
        left = jnp.concatenate([left_high, left_high, left_low], axis=1)
        message = dot(left, weight_ref[...]) + bias
        store(start, step, layer_norm(message, gain, shift_row))


def aggregate(receiver_row, nodes, normed):
    node = lax.broadcasted_iota(jnp.int32, (nodes, receiver_row.shape[1]), 0)
    onehot = jnp.where(node == receiver_row, 1.0, 0.0).astype(BF16)
    width = normed.shape[1] // 2
    both = dot(onehot, normed)
    return both[:, :width] + both[:, width:]


def per_device(
    grid_latent,
    mesh_latent,
    grid_edge_feats,
    grid_senders,
    grid_receivers,
    mesh_edge_feats,
    mesh_senders,
    mesh_receivers,
    edge_weight,
    sender_weight,
    receiver_weight,
    first_bias,
    out_weight,
    out_bias,
    norm_gain,
    norm_shift,
):
    lon_count = lax.axis_size("lon")
    hid_count = lax.axis_size("hid")
    rows, cols, width = grid_latent.shape
    nodes = mesh_latent.shape[2]
    units = sender_weight.shape[2]
    grid_edges = grid_senders.shape[2]
    mesh_edges = mesh_senders.shape[2]
    mesh_own = mesh_latent.reshape(nodes, width)
    cells = grid_latent.reshape(rows * cols, width)
    grid_ids = grid_senders.reshape(1, grid_edges)
    grid_to = grid_receivers.reshape(1, grid_edges)
    mesh_ids = mesh_senders.reshape(1, mesh_edges)
    mesh_to = mesh_receivers.reshape(1, mesh_edges)
    two_lon = lon_count == 2
    id_rows = mesh_edges // LANES
    side_size = rows * 2 * RIM
    side_rows = side_size + id_rows + -(side_size + id_rows) % 8
    lat_size = RIM * cols + RIM * 2 * RIM
    lat_rows = lat_size + id_rows + -(lat_size + id_rows) % 16

    def local(receivers):
        patch = lax.axis_index("lat") * lon_count + lax.axis_index("lon")
        return receivers - patch * nodes

    def cell_places(ids):
        lat_index = lax.axis_index("lat")
        total_lon = cols * lon_count
        row, col = divide(ids, total_lon)
        row = row - lat_index * rows
        col = divide(col - lax.axis_index("lon") * cols + RIM, total_lon)[1] - RIM
        in_rows = (row >= 0) & (row < rows)
        in_cols = (col >= 0) & (col < cols)
        own = jnp.where(in_rows & in_cols, row * cols + col, -1)
        slot = jnp.where(col < 0, col + 2 * RIM, col - cols)
        rim_row = jnp.where(row < 0, row + RIM, row - rows)
        rim = jnp.where(in_cols, rim_row * cols + col, RIM * cols + rim_row * 2 * RIM + slot)
        odd = lat_index % 2
        rim = rim + side_size + jnp.where(row < 0, 1 - odd, odd) * lat_rows
        beyond = jnp.where(in_rows, jnp.where(in_cols, -1, row * 2 * RIM + slot), rim)
        return own, beyond

    def lat_partners():
        lat_index = lax.axis_index("lat")
        turn = 1 - 2 * (lat_index % 2)
        return lat_index + turn, lat_index - turn

    def sender_nodes(ids):
        source, node = divide(ids, nodes)
        source_lat, source_lon = divide(source, lon_count)
        offset = divide(source_lon - lax.axis_index("lon") + lon_count, lon_count)[1]
        tag = source_lat * lon_count + offset
        own = lax.axis_index("lat") * lon_count
        odd = lax.axis_index("hid") % 2 == 1
        first, second = lat_partners()
        first = jnp.where(odd, first * lon_count, own + (1 if two_lon else lon_count - 1))
        second = jnp.where(odd, second * lon_count, -1 if two_lon else own + 1)
        received = jnp.where(tag == first, node, jnp.where(tag == second, node + nodes, -1))
        return jnp.where(tag == own, node, -1), received

    def choose_ids(way, lat_ref, lon_ref):
        odd = lax.axis_index("hid") % 2 == 1
        partner = lat_partners()[way]
        along_lat = jnp.where((partner >= 0) & (partner < lax.axis_size("lat")), 1, 0)
        valid = jnp.where(odd, 0 if two_lon and way == 1 else 1, along_lat)
        ids = jnp.where(odd, ids_in(lon_ref, side_size), ids_in(lat_ref, lat_size))
        return jnp.where(valid == 1, ids, -4 * nodes * lon_count)

    def ids_in(ref, start):
        rows_of = [ref[start + row : start + row + 1, :] for row in range(id_rows)]
        return jnp.concatenate(rows_of, axis=1).astype(jnp.int32)

    def put_ids(ref, start, id_ref):
        ids = id_ref[...].astype(F32)
        for row in range(id_rows):
            ref[start + row : start + row + 1, :] = ids[:, row * LANES : (row + 1) * LANES]
        end = start + id_rows
        if end < ref.shape[0]:
            ref[end:, :] = jnp.zeros((ref.shape[0] - end, units), F32)

    def side_table(low_ref, high_ref):
        if two_lon:
            return low_ref[:side_size, :]
        slot = lax.broadcasted_iota(jnp.int32, (side_size, units), 0) % (2 * RIM)
        return jnp.where(slot < RIM, high_ref[:side_size, :], low_ref[:side_size, :])

    out_pieces = gather_hid(out_weight)

    chunk = rows * cols // 4

    def terms_body(
        cell_ref, weight_ref, id_ref, term_ref, side_ref, cell_vmem, weight_vmem, id_vmem, sems
    ):
        loads = [
            pltpu.make_async_copy(weight_ref.at[0], weight_vmem, sems.at[0]),
            pltpu.make_async_copy(id_ref, id_vmem, sems.at[1]),
        ]
        for step in range(4):
            part = pl.ds(step * chunk, chunk)
            loads.append(
                pltpu.make_async_copy(cell_ref.at[part], cell_vmem.at[part], sems.at[step + 2])
            )
        for load in loads:
            load.start()
        loads[0].wait()
        for step in range(4):
            loads[step + 2].wait()
            start = step * chunk
            term_ref[start : start + chunk, :] = dot_split(
                cell_vmem[start : start + chunk, :], weight_vmem[...]
            )
        loads[1].wait()
        put_ids(side_ref, side_size, id_vmem)
        for row in range(rows):
            start = row * 2 * RIM
            side_ref[start : start + RIM, :] = term_ref[row * cols : row * cols + RIM, :]
            side_ref[start + RIM : start + 2 * RIM, :] = term_ref[
                (row + 1) * cols - RIM : (row + 1) * cols, :
            ]

    hbm = pl.BlockSpec(memory_space=pltpu.HBM)
    terms, sides = pl.pallas_call(
        terms_body,
        out_shape=(shape(rows * cols, units), shape(side_rows, units)),
        in_specs=[hbm, hbm, hbm],
        out_specs=(VMEM, VMEM),
        scratch_shapes=[
            pltpu.VMEM((rows * cols, width), F32),
            pltpu.VMEM((width, units), F32),
            pltpu.VMEM((1, mesh_edges), jnp.int32),
            pltpu.SemaphoreType.DMA((6,)),
        ],
        name="grid_terms",
        compiler_params=pltpu.CompilerParams(vmem_limit_bytes=KERNEL_VMEM),
        cost_estimate=pl.CostEstimate(
            flops=6 * rows * cols * width * units, bytes_accessed=1 << 21, transcendentals=0
        ),
    )(
        pltpu.with_memory_space_constraint(cells, pltpu.HBM),
        pltpu.with_memory_space_constraint(sender_weight, pltpu.HBM),
        pltpu.with_memory_space_constraint(mesh_ids, pltpu.HBM),
    )
    side_low = shift(sides, "lon", 1)
    side_high = side_low if two_lon else shift(sides, "lon", -1)

    def grid_own_body(term_ref, feat_ref, edge_ref, bias_ref, send_ref, out_ref):
        out_ref[...] = (
            pick(cell_places(send_ref[...])[0], term_ref[...])
            + edge_terms(feat_ref[...], edge_ref[0])
            + bias_ref[0:1, :]
        )

    grid_pre = call(
        grid_own_body,
        shape(grid_edges, units),
        8 * grid_edges * rows * cols * units,
        (terms, grid_edge_feats.reshape(-1, grid_edges), edge_weight, first_bias, grid_ids),
    )

    def grid_received_body(pre_ref, mesh_ref, weight_ref, recv_ref, out_ref):
        received = dot_split(mesh_ref[...], weight_ref[0])
        out_ref[...] = pre_ref[...] + pick(local(recv_ref[...]), received)

    grid_pre = call(
        grid_received_body,
        shape(grid_edges, units),
        8 * grid_edges * rows * cols * units,
        (grid_pre, mesh_own, receiver_weight, grid_to),
    )

    def rim_body(term_ref, low_ref, high_ref, id_ref, a_ref, b_ref):
        odd = lax.axis_index("lat") % 2
        table = side_table(low_ref, high_ref)
        for ref, up in ((a_ref, 1 - odd), (b_ref, odd)):
            start = up * (rows - RIM)
            ref[: RIM * cols, :] = term_ref[pl.ds(pl.multiple_of(start * cols, 8), RIM * cols), :]
            ref[RIM * cols : lat_size, :] = jnp.where(
                up == 1, table[(rows - RIM) * 2 * RIM :, :], table[: RIM * 2 * RIM, :]
            )
            put_ids(ref, lat_size, id_ref)

    rim_block = shape(lat_rows, units)
    rim_a, rim_b = call(rim_body, (rim_block, rim_block), 1 << 20, (terms, side_low, side_high, mesh_ids))
    rim_a = swap_lat(rim_a, 0)
    rim_b = swap_lat(rim_b, 1)

    halves = [shape(grid_edges // 2, units)] * 2

    def grid_hidden_body(pre_ref, low_ref, high_ref, a_ref, b_ref, send_ref, *hidden_refs):
        pad = -(side_size + 2 * lat_rows) % LANES
        table = jnp.concatenate(
            [side_table(low_ref, high_ref), a_ref[...], b_ref[...], jnp.zeros((pad, units), F32)],
            axis=0,
        )
        total = pre_ref[...] + pick(cell_places(send_ref[...])[1], table)
        total = total / (1.0 + jnp.exp(-total))
        for half, ref in enumerate(hidden_refs):
            ref[...] = total[half * ref.shape[0] : (half + 1) * ref.shape[0], :]

    grid_hidden = call(
        grid_hidden_body,
        tuple(halves),
        4 * grid_edges * rows * cols * units,
        (grid_pre, side_low, side_high, rim_a, rim_b, grid_ids),
    )
    grid_pieces = [gather_hid(part) for part in grid_hidden]

    def weight_body(*refs):
        for section in range(2):
            whole = jnp.concatenate([ref[section] for ref in refs[:hid_count]], axis=0)
            high, low = split(whole)
            out_ref = refs[hid_count + section]
            out_ref[:width, :] = high
            out_ref[width : 2 * width, :] = low
            out_ref[2 * width :, :] = high

    weight_block = shape(3 * width, width, dtype=BF16)
    grid_weight, mesh_weight = call(weight_body, (weight_block, weight_block), 1 << 28, out_pieces)

    half_edges = grid_edges // 2

    def half_sum(half, refs, normed_ref):
        hidden_refs = refs[:hid_count]
        weight_ref, bias_ref, gain_ref, shift_ref, recv_ref = refs[hid_count : hid_count + 5]

        def store(start, step, normed):
            high, low = split(normed)
            normed_ref[start : start + step, :width] = high
            normed_ref[start : start + step, width:] = low

        normed_chunks(
            hidden_refs, weight_ref, bias_ref[0:1, :], gain_ref[0:1, :], shift_ref[0:1, :], store
        )
        receivers = recv_ref[:, half * half_edges : (half + 1) * half_edges]
        return aggregate(local(receivers), nodes, normed_ref[...])

    def grid_first_half_body(*refs):
        mesh_ref, sum_ref, normed_ref = refs[-3:]
        sum_ref[...] = mesh_ref[...] + half_sum(0, refs, normed_ref)

    def grid_second_half_body(*refs):
        first_ref, send_ref, mid_ref, term_ref, normed_ref = refs[-5:]
        middle = first_ref[...] + half_sum(1, refs, normed_ref)
        mid_ref[...] = middle
        term_ref[...] = dot_split(middle, send_ref[1])

    normed_scratch = (pltpu.VMEM((half_edges, 2 * width), BF16),)
    shared = (grid_weight, out_bias, norm_gain, norm_shift, grid_to)
    first_sum = call(
        grid_first_half_body,
        shape(nodes, width),
        5 * grid_edges * width * width,
        (*grid_pieces[0], *shared, mesh_own),
        normed_scratch,
    )
    mesh_mid, mesh_terms = call(
        grid_second_half_body,
        (shape(nodes, width), shape(nodes, units)),
        6 * grid_edges * width * width,
        (*grid_pieces[1], *shared, first_sum, sender_weight),
        normed_scratch,
    )

    back = None if two_lon else -1
    table_a = by_role(mesh_terms, 0, 1, 0)
    table_b = by_role(mesh_terms, 0, back, 1)

    def mesh_first_body(
        term_ref, mid_ref, weight_ref, feat_ref, edge_ref, bias_ref, recv_ref, id_ref,
        rim_a_ref, rim_b_ref, low_ref, high_ref, pre_ref, a_ref, b_ref, hot_ref,
    ):
        table = term_ref[...]
        own_a, received_a = sender_nodes(choose_ids(0, rim_a_ref, high_ref))
        own_b, received_b = sender_nodes(choose_ids(1, rim_b_ref, low_ref))
        a_ref[...] = pick(own_a, table)
        b_ref[...] = pick(own_b, table)
        hot_ref[:mesh_edges, :] = onehot_rows(down_lanes(received_a), 2 * nodes)
        hot_ref[mesh_edges:, :] = onehot_rows(down_lanes(received_b), 2 * nodes)
        received = dot_split(mid_ref[...], weight_ref[1])
        pre_ref[...] = (
            pick(sender_nodes(id_ref[...])[0], table)
            + pick(local(recv_ref[...]), received)
            + edge_terms(feat_ref[...], edge_ref[1])
            + bias_ref[1:2, :]
        )

    edge_block = shape(mesh_edges, units)
    mesh_pre, send_a, send_b, sent_hot = call(
        mesh_first_body,
        (edge_block, edge_block, edge_block, shape(2 * mesh_edges, 2 * nodes, dtype=BF16)),
        16 * mesh_edges * nodes * units,
        (
            mesh_terms, mesh_mid, receiver_weight, mesh_edge_feats.reshape(-1, mesh_edges), edge_weight,
            first_bias, mesh_to, mesh_ids, rim_a, rim_b, side_low, side_high,
        ),
    )

    def mesh_sent_body(table_a_ref, table_b_ref, first_a, first_b, hot_ref, a_ref, b_ref):
        table = jnp.concatenate([table_a_ref[...], table_b_ref[...]], axis=0)
        rows_of = pick_hot(hot_ref[...], table)
        a_ref[...] = first_a[...] + rows_of[:mesh_edges, :]
        b_ref[...] = first_b[...] + rows_of[mesh_edges:, :]

    send_a, send_b = call(
        mesh_sent_body,
        (edge_block, edge_block),
        16 * mesh_edges * nodes * units,
        (table_a, table_b, send_a, send_b, sent_hot),
    )
    got_a = by_role(send_a, 1, 1, 0)
    got_b = by_role(send_b, 1, back, 1)

    def mesh_own_body(table_a_ref, table_b_ref, first_ref, id_ref, out_ref):
        table = jnp.concatenate([table_a_ref[...], table_b_ref[...]], axis=0)
        out_ref[...] = first_ref[...] + pick(sender_nodes(id_ref[...])[1], table)

    mesh_pre = call(mesh_own_body, edge_block, 8 * mesh_edges * nodes * units, (table_a, table_b, mesh_pre, mesh_ids))
    total = mesh_pre + got_a + got_b
    mesh_pieces = gather_hid(total / (1.0 + jnp.exp(-total)))
    share = width // hid_count

    def mesh_message_body(*refs):
        hidden_refs = refs[:hid_count]
        weight_ref, bias_ref, gain_ref, shift_ref, recv_ref, mid_ref, out_ref, normed_ref = refs[hid_count:]
        place = lax.axis_index("hid")

        def own_part(value):
            part = value[:, :share]
            for step in range(1, hid_count):
                part = jnp.where(place == step, value[:, step * share : (step + 1) * share], part)
            return part

        def store(start, step, normed):
            high, low = split(own_part(normed))
            normed_ref[start : start + step, :share] = high
            normed_ref[start : start + step, share:] = low

        normed_chunks(
            hidden_refs, weight_ref, bias_ref[1:2, :], gain_ref[1:2, :], shift_ref[1:2, :], store
        )
        out_ref[...] = own_part(mid_ref[...]) + aggregate(local(recv_ref[...]), nodes, normed_ref[...])

    mesh_out = call(
        mesh_message_body,
        shape(nodes, share),
        8 * mesh_edges * width * width,
        (*mesh_pieces, mesh_weight, out_bias, norm_gain, norm_shift, mesh_to, mesh_mid),
        (pltpu.VMEM((mesh_edges, 2 * share), BF16),),
    )
    return mesh_out.reshape(1, 1, nodes, share)


def solution(mesh):
    return jax.shard_map(
        per_device,
        mesh=mesh,
        in_specs=(
            P("lat", "lon", None),
            P("lat", "lon", None, None),
            P("lat", "lon", None, None),
            P("lat", "lon", None),
            P("lat", "lon", None),
            P("lat", "lon", None, None),
            P("lat", "lon", None),
            P("lat", "lon", None),
            P(None, None, "hid"),
            P(None, None, "hid"),
            P(None, None, "hid"),
            P(None, "hid"),
            P(None, "hid", None),
            P(),
            P(),
            P(),
        ),
        out_specs=P("lat", "lon", None, "hid"),
        check_vma=False,
    )
```
